128 devices in a mesh: bank: 4 (over x_hi, core), lane: 32 (over z, y, x_lo).
Axes of the slice: x: 4 (x_hi: 2, x_lo: 2; x = x_hi * 2 + x_lo), y: 4, z: 4, core: 2. Of those that a mesh axis runs over, the one named last changes fastest.
Arguments:
- amplitudes: float32 [2, 1024, 128, 128], P(None, ('bank', 'lane')), may hold values from -6 to 6
- energies: float32 [1024, 128, 128], P(('bank', 'lane')), may hold values from -2 to 2
- diagonal_angles: float32 [2, 128], replicated, may hold values from 0.3 to 1.2
Outputs:
- final_parts: float32 [2, 1024, 128, 128], P(None, ('bank', 'lane'))
- marginal: float32 [256, 128, 128], P('lane', 'bank')
The draws below stay inside these ranges and needn't reach their ends.
All inputs are finite; a program needn't handle non-finite values.
Results may differ from the reference program's by a relative error of at most 0.0003.
Values sent between devices are 32-bit elements; how exact they have to be, the bound alone decides.
No kernel may reach another device: no remote copies, remote signals or barrier semaphores. Data moves between devices by JAX's collectives and lax.ppermute only.
A program may use at most 64 MiB of HBM per device.

```python
import jax
import jax.numpy as jnp
from jax import lax

BLOCKS_DEV = 8
ROWS = 128
LANES = 128
BLOCKS = 1024
LAYERS = 2
N_BANK = 4
N_LANE = 32


def block_scale(stream_key, dims, pieces, smallest, high):
    loudness, own = 1.0, jax.random.fold_in(stream_key, 6)
    for position, blocks in pieces:
        heights = jnp.exp(jax.random.uniform(jax.random.fold_in(own, position), (blocks,), jnp.float32, smallest / len(pieces), high / len(pieces)))
        loudness = loudness * jnp.repeat(heights, dims[position] // blocks).reshape([-1 if axis == position else 1 for axis in range(len(dims))])
    return loudness


def normal_values(key, shape, width, most, shards=(), held_as=jnp.bfloat16):
    drawn = width * jax.random.normal(key, shape, jnp.float32)
    if shards:
        drawn = drawn * block_scale(key, shape, shards, -0.22, 0.18)
    return jnp.clip(drawn, -most, most).astype(held_as)


def setup_inputs(seed: int = 0) -> dict:
    splits = jax.random.split(jax.random.key(seed), 4)
    return {
        "amplitudes": normal_values(splits[0], (2, BLOCKS, ROWS, LANES), 1.0, 6.0, ((1, 128),), jnp.float32),
        "energies": jnp.clip(jax.random.uniform(splits[1], (BLOCKS, ROWS, LANES), jnp.float32, -2.0, 2.0) * block_scale(splits[1], (BLOCKS, ROWS, LANES), ((0, 128),), -0.4, 0.0), -2.0, 2.0),
        "diagonal_angles": jnp.clip(jax.random.uniform(splits[2], (LAYERS, LANES), jnp.float32, 0.3, 1.2), 0.3, 1.2),
    }


def count_bits(values, count):
    places = jnp.arange(count.bit_length() - 1, dtype=jnp.int32)
    return jnp.sum((values[..., None] >> places) & 1, axis=-1)


def walsh_table(count):
    rank = jnp.arange(count, dtype=jnp.int32)
    parity = count_bits(rank[:, None] & rank[None, :], count) % 2
    real_part = jnp.where(parity == 1, -1.0, 1.0).astype(jnp.float32) * (count ** -0.5)
    return real_part


def apply_along(values, dim):
    real_part = walsh_table(values.shape[dim])
    def times(table):
        moved = jnp.tensordot(values, table, axes=([dim], [0]), precision=lax.Precision.HIGHEST)
        return jnp.moveaxis(moved, -1, dim)
    return times(real_part)


def diagonal_step(values, levels, angle):
    turn = angle * levels
    return jnp.stack([values[0] * jnp.cos(turn) + values[1] * jnp.sin(turn), values[1] * jnp.cos(turn) - values[0] * jnp.sin(turn)])


def reference(amplitudes, energies, diagonal_angles):
    values = amplitudes
    for layer in range(LAYERS):
        values = diagonal_step(values, energies, diagonal_angles[layer])
        values = apply_along(values, 3)
        values = apply_along(values, 2)
        parts = values.reshape(2, N_BANK, N_LANE, BLOCKS_DEV, ROWS, LANES)
        parts = apply_along(parts, 1)
        parts = apply_along(parts, 2)
        parts = apply_along(parts, 3)
        values = parts.reshape(values.shape)
    chance = values[0] * values[0] + values[1] * values[1]
    marginal = jnp.mean(chance.reshape(N_BANK, -1, ROWS, LANES), axis=0)
    return values, marginal
```

```python
import functools

import jax
import jax.numpy as jnp
import numpy as np
from jax import lax
from jax.experimental import pallas as pl
from jax.experimental.pallas import tpu as pltpu
from jax.sharding import PartitionSpec as P

F32 = jnp.float32
BF16 = jnp.bfloat16
HALF = 2.0**-12


def fit(parity, terms, reach=2.6):
    k = np.arange(400)
    x = reach * np.cos(np.pi * (k + 0.5) / 400)
    powers = np.stack([x ** (2 * n + parity) for n in range(terms)], 1)
    want = np.sin(x) if parity else np.cos(x)
    scale = np.abs(powers).max(0)
    coef = np.linalg.lstsq(powers / scale, want, rcond=None)[0] / scale
    return [float(c) for c in coef]


SIN, COS = fit(1, 7), fit(0, 8)


def horner(coefs, x2):
    total = jnp.full_like(x2, coefs[-1])
    for c in coefs[-2::-1]:
        total = total * x2 + c
    return total


def turned(re, im, turn):
    x2 = turn * turn
    sin, cos = turn * horner(SIN, x2), horner(COS, x2)
    return re * cos + im * sin, im * cos - re * sin


def walsh(parts):
    parts, step = list(parts), 1
    while step < len(parts):
        for i in range(len(parts)):
            if not i & step:
                u, v = parts[i], parts[i + step]
                parts[i], parts[i + step] = u + v, u - v
        step *= 2
    return parts


def signs():
    both = lax.broadcasted_iota(jnp.int32, (128, 128), 0) & lax.broadcasted_iota(jnp.int32, (128, 128), 1)
    for shift in (4, 2, 1):
        both = both ^ (both >> shift)
    return (1 - 2 * (both & 1)).astype(F32).astype(BF16)


def split(x):
    first = x.astype(BF16)
    rest = x - first.astype(F32)
    second = rest.astype(BF16)
    third = (rest - second.astype(F32)).astype(BF16)
    return [first, second, third]


def mixed(re, im, sign):
    both = jnp.concatenate([re, im], 0)
    right = jnp.concatenate([sign] * 3, 0)
    both = jnp.dot(jnp.concatenate(split(both), 1), right, preferred_element_type=F32)
    both = jnp.concatenate([both[:128], both[128:]], 1)
    left = jnp.concatenate([sign] * 3, 1)
    both = jnp.dot(left, jnp.concatenate(split(both), 0), preferred_element_type=F32)
    return both[:, :128], both[:, 128:]


def first_kernel(amp, ener, angle, out):
    sign = signs()
    a = angle[0:1, :]
    for b in range(8):
        e = ener[b]
        re, im = turned(amp[0, b], amp[1, b], a * e)
        re, im = mixed(re, im, sign)
        out[b * 16 : b * 16 + 16, 0] = re.reshape(16, 8, 128)
        out[b * 16 : b * 16 + 16, 1] = im.reshape(16, 8, 128)
        out[b * 16 : b * 16 + 16, 2] = e.reshape(16, 8, 128)
    for r in range(16):
        for c in range(2):
            for b, part in enumerate(walsh([out[b * 16 + r, c] for b in range(8)])):
                out[b * 16 + r, c] = part


def second_kernel(got, angle, out):
    sign = signs()
    a = angle[1:2, :]
    for r in range(16):
        for c in range(2):
            for b, part in enumerate(walsh([got[b * 16 + r, c] for b in range(8)])):
                out[b * 16 + r, c] = part
    for b in range(8):
        rows = range(b * 16, b * 16 + 16)
        re = jnp.concatenate(walsh([out[r, 0] for r in rows]), 0)
        im = jnp.concatenate(walsh([out[r, 1] for r in rows]), 0)
        e = got[b * 16 : b * 16 + 16, 2].reshape(128, 128)
        re, im = turned(re * HALF, im * HALF, a * e)
        re, im = mixed(re, im, sign)
        out[b * 16 : b * 16 + 16, 0] = re.reshape(16, 8, 128)
        out[b * 16 : b * 16 + 16, 1] = im.reshape(16, 8, 128)
    for r in range(16):
        for c in range(2):
            for b, part in enumerate(walsh([out[b * 16 + r, c] for b in range(8)])):
                out[b * 16 + r, c] = part


def third_kernel(core, got, out, keep, send, held):
    for b in range(8):
        for c in range(2):
            rows = range(b * 16, b * 16 + 16)
            for r, part in zip(rows, walsh([got[r, c] * HALF for r in rows])):
                held[r, c] = part
    mine = core[0] == 0
    for hi in range(2):
        for low in range(4):
            chance = [[], []]
            for co in range(2):
                r = hi * 8 + co * 4 + low
                re = walsh([held[b * 16 + r, 0] for b in range(8)])
                im = walsh([held[b * 16 + r, 1] for b in range(8)])
                for b in range(8):
                    out[0, b, r * 8 : r * 8 + 8, :] = re[b]
                    out[1, b, r * 8 : r * 8 + 8, :] = im[b]
                    chance[co].append((re[b] * re[b] + im[b] * im[b]) * 0.25)
            for b in range(8):
                u, v = chance[0][b], chance[1][b]
                keep[hi, b, low * 8 : low * 8 + 8, :] = jnp.where(mine, u, v)
                send[hi, b, low * 8 : low * 8 + 8, :] = jnp.where(mine, v, u)


def shape(*dims):
    return jax.ShapeDtypeStruct(dims, F32)


VMEM = pl.BlockSpec(memory_space=pltpu.VMEM)
SMEM = pl.BlockSpec(memory_space=pltpu.SMEM)
BOTH = ("bank", "lane")


def shards(amplitudes, energies, diagonal_angles):
    bank = lax.axis_index("bank")
    values = pl.pallas_call(
        first_kernel, out_shape=shape(128, 3, 8, 128), in_specs=[VMEM] * 3, out_specs=VMEM, name="first"
    )(amplitudes, energies, diagonal_angles)
    values = lax.all_to_all(values.reshape(128, 24, 128), BOTH, 0, 0, tiled=True)
    values = pl.pallas_call(
        second_kernel, out_shape=shape(128, 2, 8, 128), in_specs=[VMEM] * 2, out_specs=VMEM, name="second"
    )(values.reshape(128, 3, 8, 128), diagonal_angles)
    values = lax.all_to_all(values.reshape(128, 16, 128), BOTH, 0, 0, tiled=True)
    final, keep, send = pl.pallas_call(
        third_kernel,
        out_shape=(shape(2, 8, 128, 128), shape(2, 8, 32, 128), shape(2, 8, 32, 128)),
        in_specs=[SMEM, VMEM],
        out_specs=(VMEM, VMEM, VMEM),
        scratch_shapes=[pltpu.VMEM((128, 2, 8, 128), F32)],
        name="third",
    )((bank % 2).reshape(1), values.reshape(128, 2, 8, 128))
    got = lax.ppermute(send, "bank", [(i, i ^ 1) for i in range(4)])
    far = bank // 2
    pick = lambda x, i: lax.dynamic_index_in_dim(x, i, 0, keepdims=False)
    away = pick(keep, 1 - far) + pick(got, 1 - far)
    here = pick(keep, far) + pick(got, far)
    marginal = here + lax.ppermute(away, "bank", [(i, i ^ 2) for i in range(4)])
    return final, marginal


def solution(mesh):
    return jax.shard_map(
        shards,
        mesh=mesh,
        in_specs=(P(None, BOTH, None, None), P(BOTH, None, None), P()),
        out_specs=(P(None, BOTH, None, None), P("lane", "bank", None)),
        check_vma=False,
    )
```

```python
import jax
import jax.numpy as jnp
import numpy as np
from jax import lax
from jax.experimental import pallas as pl
from jax.experimental.pallas import tpu as pltpu
from jax.sharding import PartitionSpec as P

F32 = jnp.float32
BF16 = jnp.bfloat16
HALF = 2.0**-12


def fit(parity, terms, reach=2.6):
    k = np.arange(400)
    x = reach * np.cos(np.pi * (k + 0.5) / 400)
    powers = np.stack([x ** (2 * n + parity) for n in range(terms)], 1)
    want = np.sin(x) if parity else np.cos(x)
    scale = np.abs(powers).max(0)
    coef = np.linalg.lstsq(powers / scale, want, rcond=None)[0] / scale
    return [float(c) for c in coef]


SIN, COS = fit(1, 7), fit(0, 8)


def horner(coefs, x2):
    total = jnp.full_like(x2, coefs[-1])
    for c in coefs[-2::-1]:
        total = total * x2 + c
    return total


def turned(re, im, turn):
    x2 = turn * turn
    sin, cos = turn * horner(SIN, x2), horner(COS, x2)
    return re * cos + im * sin, im * cos - re * sin


def walsh(parts):
    parts, step = list(parts), 1
    while step < len(parts):
        for i in range(len(parts)):
            if not i & step:
                u, v = parts[i], parts[i + step]
                parts[i], parts[i + step] = u + v, u - v
        step *= 2
    return parts


def signs():
    both = lax.broadcasted_iota(jnp.int32, (128, 128), 0) & lax.broadcasted_iota(jnp.int32, (128, 128), 1)
    for shift in (4, 2, 1):
        both = both ^ (both >> shift)
    return (1 - 2 * (both & 1)).astype(F32).astype(BF16)


def split(x):
    first = x.astype(BF16)
    rest = x - first.astype(F32)
    second = rest.astype(BF16)
    third = (rest - second.astype(F32)).astype(BF16)
    return [first, second, third]


def mixed(re, im, sign):
    both = jnp.concatenate([re, im], 0)
    right = jnp.concatenate([sign] * 3, 0)
    both = jnp.dot(jnp.concatenate(split(both), 1), right, preferred_element_type=F32)
    both = jnp.concatenate([both[:128], both[128:]], 1)
    left = jnp.concatenate([sign] * 3, 1)
    both = jnp.dot(left, jnp.concatenate(split(both), 0), preferred_element_type=F32)
    return both[:, :128], both[:, 128:]


def first_kernel(amp, ener, angle, out, arrived):
    def copies(b):
        rows = pl.ds(b * 16, 16)
        return [
            pltpu.make_async_copy(amp.at[0, b], out.at[rows, 0], arrived.at[b, 0]),
            pltpu.make_async_copy(amp.at[1, b], out.at[rows, 1], arrived.at[b, 1]),
            pltpu.make_async_copy(ener.at[b], out.at[rows, 2], arrived.at[b, 2]),
        ]

    for b in range(8):
        for copy in copies(b):
            copy.start()
    sign = signs()
    a = angle[0:1, :]
    for b in range(8):
        for copy in copies(b):
            copy.wait()
        re, im, e = (out[b * 16 : b * 16 + 16, c].reshape(128, 128) for c in range(3))
        re, im = turned(re, im, a * e)
        re, im = mixed(re, im, sign)
        out[b * 16 : b * 16 + 16, 0] = re.reshape(16, 8, 128)
        out[b * 16 : b * 16 + 16, 1] = im.reshape(16, 8, 128)
    for r in range(16):
        for c in range(2):
            for b, part in enumerate(walsh([out[b * 16 + r, c] for b in range(8)])):
                out[b * 16 + r, c] = part


def second_kernel(got, angle, out):
    sign = signs()
    a = angle[1:2, :]
    for r in range(16):
        for c in range(2):
            for b, part in enumerate(walsh([got[b * 16 + r, c] for b in range(8)])):
                out[b * 16 + r, c] = part
    for b in range(8):
        rows = range(b * 16, b * 16 + 16)
        re = jnp.concatenate(walsh([out[r, 0] for r in rows]), 0)
        im = jnp.concatenate(walsh([out[r, 1] for r in rows]), 0)
        e = got[b * 16 : b * 16 + 16, 2].reshape(128, 128)
        re, im = turned(re * HALF, im * HALF, a * e)
        re, im = mixed(re, im, sign)
        out[b * 16 : b * 16 + 16, 0] = re.reshape(16, 8, 128)
        out[b * 16 : b * 16 + 16, 1] = im.reshape(16, 8, 128)
    for r in range(16):
        for c in range(2):
            for b, part in enumerate(walsh([out[b * 16 + r, c] for b in range(8)])):
                out[b * 16 + r, c] = part


def third_kernel(place, got, out, keep, send, held):
    for r in range(16):
        for c in range(2):
            for b, part in enumerate(walsh([got[b * 16 + r, c] * HALF for b in range(8)])):
                held[b * 16 + r, c] = part
    mine = (place[0] & 1) == 0
    far = place[0] >> 1
    for b in range(8):
        chance = []
        re = walsh([held[b * 16 + r, 0] for r in range(16)])
        im = walsh([held[b * 16 + r, 1] for r in range(16)])
        for r in range(16):
            out[0, b, r * 8 : r * 8 + 8, :] = re[r]
            out[1, b, r * 8 : r * 8 + 8, :] = im[r]
            chance.append((re[r] * re[r] + im[r] * im[r]) * 0.25)
        for hi in range(2):
            for low in range(4):
                u, v = chance[hi * 8 + low], chance[hi * 8 + 4 + low]
                keep[hi ^ far, b, low * 8 : low * 8 + 8, :] = jnp.where(mine, u, v)
                send[hi ^ far, b, low * 8 : low * 8 + 8, :] = jnp.where(mine, v, u)


def here(*dims):
    return pltpu.VMEM(dims, F32)


def near(x):
    return pltpu.with_memory_space_constraint(x, pltpu.VMEM)


VMEM = pl.BlockSpec(memory_space=pltpu.VMEM)
SMEM = pl.BlockSpec(memory_space=pltpu.SMEM)
HBM = pl.BlockSpec(memory_space=pltpu.HBM)
BOTH = ("bank", "lane")
ORDER = ("lane", "bank")


def shards(amplitudes, energies, diagonal_angles):
    diagonal_angles, bank = lax.optimization_barrier((diagonal_angles, lax.axis_index("bank")))
    values = pl.pallas_call(
        first_kernel,
        out_shape=here(128, 3, 8, 128),
        in_specs=[HBM, HBM, VMEM],
        out_specs=VMEM,
        scratch_shapes=[pltpu.SemaphoreType.DMA((8, 3))],
        name="first",
    )(amplitudes.reshape(2, 8, 16, 8, 128), energies.reshape(8, 16, 8, 128), diagonal_angles)
    values = lax.all_to_all(values.reshape(128, 24, 128), ORDER, 0, 0, tiled=True)
    values = pl.pallas_call(
        second_kernel, out_shape=here(128, 2, 8, 128), in_specs=[VMEM] * 2, out_specs=VMEM, name="second"
    )(near(values.reshape(128, 3, 8, 128)), diagonal_angles)
    values = lax.all_to_all(values.reshape(128, 16, 128), ORDER, 0, 0, tiled=True)
    final, keep, send = pl.pallas_call(
        third_kernel,
        out_shape=(here(2, 8, 128, 128), here(2, 8, 32, 128), here(2, 8, 32, 128)),
        in_specs=[SMEM, VMEM],
        out_specs=(VMEM, VMEM, VMEM),
        scratch_shapes=[pltpu.VMEM((128, 2, 8, 128), F32)],
        name="third",
    )(bank.reshape(1), near(values.reshape(128, 2, 8, 128)))
    got = lax.ppermute(send, "bank", [(i, i ^ 1) for i in range(4)])
    marginal = keep[0] + got[0] + lax.ppermute(keep[1] + got[1], "bank", [(i, i ^ 2) for i in range(4)])
    return final, marginal


def solution(mesh):
    return jax.shard_map(
        shards,
        mesh=mesh,
        in_specs=(P(None, BOTH, None, None), P(BOTH, None, None), P()),
        out_specs=(P(None, BOTH, None, None), P("lane", "bank", None)),
        check_vma=False,
    )
```

```python
import jax
import jax.numpy as jnp
import numpy as np
from jax import lax
from jax.experimental import pallas as pl
from jax.experimental.pallas import tpu as pltpu
from jax.sharding import PartitionSpec as P

F32 = jnp.float32
BF16 = jnp.bfloat16
GROUP = 4
HALF = 2.0**-12


def fit(parity, terms, reach=2.6):
    k = np.arange(400)
    x = reach * np.cos(np.pi * (k + 0.5) / 400)
    powers = np.stack([x ** (2 * n + parity) for n in range(terms)], 1)
    want = np.sin(x) if parity else np.cos(x)
    scale = np.abs(powers).max(0)
    coef = np.linalg.lstsq(powers / scale, want, rcond=None)[0] / scale
    return [float(c) for c in coef]


SIN, COS = fit(1, 7), fit(0, 8)


def horner(coefs, x2):
    total = jnp.full_like(x2, coefs[-1])
    for c in coefs[-2::-1]:
        total = total * x2 + c
    return total


def turned(re, im, turn):
    x2 = turn * turn
    sin, cos = turn * horner(SIN, x2), horner(COS, x2)
    return re * cos + im * sin, im * cos - re * sin


def walsh(parts):
    parts, step = list(parts), 1
    while step < len(parts):
        for i in range(len(parts)):
            if not i & step:
                u, v = parts[i], parts[i + step]
                parts[i], parts[i + step] = u + v, u - v
        step *= 2
    return parts


def signs():
    both = lax.broadcasted_iota(jnp.int32, (128, 128), 0) & lax.broadcasted_iota(jnp.int32, (128, 128), 1)
    for shift in (4, 2, 1):
        both = both ^ (both >> shift)
    return (1 - 2 * (both & 1)).astype(F32).astype(BF16)


PIECES = 3


def mixed(re, im, sign):
    rest = jnp.concatenate([re, im], 0)
    pieces = []
    for _ in range(PIECES):
        pieces.append(rest.astype(BF16))
        rest = rest - pieces[-1].astype(F32)
    both = jnp.dot(jnp.concatenate(pieces, 1), jnp.concatenate([sign] * PIECES, 0), preferred_element_type=F32)
    return both[:128], both[128:]


def tiles(x):
    return [x[r * 8 : r * 8 + 8] for r in range(x.shape[0] // 8)]


def first_kernel(amp, ener, angle, out, held, state, arrived):
    def copies(b):
        return [
            pltpu.make_async_copy(amp.at[0, b], held.at[b, 0], arrived.at[b, 0]),
            pltpu.make_async_copy(amp.at[1, b], held.at[b, 1], arrived.at[b, 1]),
            pltpu.make_async_copy(ener.at[b], held.at[b, 2], arrived.at[b, 2]),
        ]

    for b in range(8):
        for copy in copies(b):
            copy.start()
    sign = signs()
    a = angle[0:1, :]
    for b in range(8):
        if b % GROUP == 0:
            for near_by in range(b, b + GROUP):
                for copy in copies(near_by):
                    copy.wait()
        re, im = turned(held[b, 0], held[b, 1], a * held[b, 2])
        for c, part in enumerate(mixed(re, im, sign)):
            for r, tile in enumerate(walsh(tiles(part))):
                state[b * 2 + c, r * 8 : r * 8 + 8, :] = tile
        for top in range(2):
            for low in range(8):
                out[b * 16 + top * 8 + low, 2] = held[b, 2, pl.ds(top * 64 + low, 8, stride=8), :]
            for c in range(2):
                rows = [state[b * 2 + c, pl.ds(top * 64 + low, 8, stride=8), :] for low in range(8)]
                for low, tile in enumerate(walsh(rows)):
                    out[b * 16 + top * 8 + low, c] = tile
    for r in range(16):
        for c in range(2):
            for b, tile in enumerate(walsh([out[b * 16 + r, c] for b in range(8)])):
                out[b * 16 + r, c] = tile


def second_kernel(got, angle, out):
    sign = signs()
    a = angle[1:2, :]
    for r in range(16):
        for c in range(2):
            for b, tile in enumerate(walsh([got[b * 16 + r, c] * HALF for b in range(8)])):
                out[b * 16 + r, c] = tile
    for b in range(8):
        rows = range(b * 16, b * 16 + 16)
        re = jnp.concatenate(walsh([out[r, 0] for r in rows]), 0)
        im = jnp.concatenate(walsh([out[r, 1] for r in rows]), 0)
        e = got[b * 16 : b * 16 + 16, 2].reshape(128, 128)
        re, im = turned(re, im, a * e)
        for c, part in enumerate(mixed(re, im, sign)):
            for r, tile in zip(rows, walsh(tiles(part))):
                out[r, c] = tile
    for r in range(16):
        for c in range(2):
            for b, tile in enumerate(walsh([out[b * 16 + r, c] for b in range(8)])):
                out[b * 16 + r, c] = tile


def third_kernel(place, got, out, keep, send, held, state):
    for r in range(16):
        for c in range(2):
            for b, tile in enumerate(walsh([got[b * 16 + r, c] * HALF for b in range(8)])):
                held[b * 16 + r, c] = tile
    mine = (place[0] & 1) == 0
    far = place[0] >> 1
    for b in range(8):
        final = []
        for c in range(2):
            for r, tile in enumerate(walsh([held[b * 16 + r, c] for r in range(16)])):
                state[b * 2 + c, pl.ds(r // 8 * 64 + r % 8, 8, stride=8), :] = tile
            both = []
            for top in range(2):
                both += walsh([state[b * 2 + c, top * 64 + mid * 8 : top * 64 + mid * 8 + 8, :] for mid in range(8)])
            for r, tile in enumerate(both):
                out[c, b, r * 8 : r * 8 + 8, :] = tile
            final.append(both)
        chance = [(re * re + im * im) * 0.25 for re, im in zip(*final)]
        for hi in range(2):
            for low in range(4):
                u, v = chance[hi * 8 + low], chance[hi * 8 + 4 + low]
                keep[hi ^ far, b, low * 8 : low * 8 + 8, :] = jnp.where(mine, u, v)
                send[hi ^ far, b, low * 8 : low * 8 + 8, :] = jnp.where(mine, v, u)


def here(*dims):
    return pltpu.VMEM(dims, F32)


def near(x):
    return pltpu.with_memory_space_constraint(x, pltpu.VMEM)


VMEM = pl.BlockSpec(memory_space=pltpu.VMEM)
SMEM = pl.BlockSpec(memory_space=pltpu.SMEM)
HBM = pl.BlockSpec(memory_space=pltpu.HBM)
BOTH = ("bank", "lane")
ORDER = ("lane", "bank")


def shards(amplitudes, energies, diagonal_angles):
    diagonal_angles, bank = lax.optimization_barrier((diagonal_angles, lax.axis_index("bank")))
    values = pl.pallas_call(
        first_kernel,
        out_shape=here(128, 3, 8, 128),
        in_specs=[HBM, HBM, VMEM],
        out_specs=VMEM,
        scratch_shapes=[here(8, 3, 128, 128), here(16, 128, 128), pltpu.SemaphoreType.DMA((8, 3))],
        name="first",
    )(amplitudes, energies, diagonal_angles)
    values = lax.all_to_all(values.reshape(128, 24, 128), ORDER, 0, 0, tiled=True)
    values = pl.pallas_call(
        second_kernel, out_shape=here(128, 2, 8, 128), in_specs=[VMEM] * 2, out_specs=VMEM, name="second"
    )(near(values.reshape(128, 3, 8, 128)), diagonal_angles)
    values = lax.all_to_all(values.reshape(128, 16, 128), ORDER, 0, 0, tiled=True)
    final, keep, send = pl.pallas_call(
        third_kernel,
        out_shape=(here(2, 8, 128, 128), here(2, 8, 32, 128), here(2, 8, 32, 128)),
        in_specs=[SMEM, VMEM],
        out_specs=(VMEM, VMEM, VMEM),
        scratch_shapes=[here(128, 2, 8, 128), here(16, 128, 128)],
        name="third",
    )(bank.reshape(1), near(values.reshape(128, 2, 8, 128)))
    got = lax.ppermute(send, "bank", [(i, i ^ 1) for i in range(4)])
    marginal = keep[0] + got[0] + lax.ppermute(keep[1] + got[1], "bank", [(i, i ^ 2) for i in range(4)])
    return final, marginal


def solution(mesh):
    return jax.shard_map(
        shards,
        mesh=mesh,
        in_specs=(P(None, BOTH, None, None), P(BOTH, None, None), P()),
        out_specs=(P(None, BOTH, None, None), P("lane", "bank", None)),
        check_vma=False,
    )
```

```python
import jax
import jax.numpy as jnp
import numpy as np
from jax import lax
from jax.experimental import pallas as pl
from jax.experimental.pallas import tpu as pltpu
from jax.sharding import PartitionSpec as P


F32 = jnp.float32
BF16 = jnp.bfloat16
GROUP = 4
HALF = 2.0**-12


def fit(parity, terms, reach=2.6):
    k = np.arange(400)
    x = reach * np.cos(np.pi * (k + 0.5) / 400)
    powers = np.stack([x ** (2 * n + parity) for n in range(terms)], 1)
    want = np.sin(x) if parity else np.cos(x)
    scale = np.abs(powers).max(0)
    coef = np.linalg.lstsq(powers / scale, want, rcond=None)[0] / scale
    return [float(c) for c in coef]


SIN, COS = fit(1, 7), fit(0, 8)


def horner(coefs, x2):
    total = jnp.full_like(x2, coefs[-1])
    for c in coefs[-2::-1]:
        total = total * x2 + c
    return total


def turned(re, im, turn):
    x2 = turn * turn
    sin, cos = turn * horner(SIN, x2), horner(COS, x2)
    return re * cos + im * sin, im * cos - re * sin


def walsh(parts):
    parts, step = list(parts), 1
    while step < len(parts):
        for i in range(len(parts)):
            if not i & step:
                u, v = parts[i], parts[i + step]
                parts[i], parts[i + step] = u + v, u - v
        step *= 2
    return parts


def signs():
    both = lax.broadcasted_iota(jnp.int32, (128, 128), 0) & lax.broadcasted_iota(jnp.int32, (128, 128), 1)
    for shift in (4, 2, 1):
        both = both ^ (both >> shift)
    return (1 - 2 * (both & 1)).astype(F32).astype(BF16)


PIECES = 3


def mixed(re, im, sign):
    rest = jnp.concatenate([re, im], 0)
    pieces = []
    for _ in range(PIECES):
        pieces.append(rest.astype(BF16))
        rest = rest - pieces[-1].astype(F32)
    both = jnp.dot(jnp.concatenate(pieces, 1), jnp.concatenate([sign] * PIECES, 0), preferred_element_type=F32)
    return both[:128], both[128:]


def tiles(x):
    return [x[r * 8 : r * 8 + 8] for r in range(x.shape[0] // 8)]


def first_kernel(amp, ener, angle, out, held, state, arrived):
    def copies(b):
        return [
            pltpu.make_async_copy(amp.at[0, b], held.at[b, 0], arrived.at[b, 0]),
            pltpu.make_async_copy(amp.at[1, b], held.at[b, 1], arrived.at[b, 1]),
            pltpu.make_async_copy(ener.at[b], held.at[b, 2], arrived.at[b, 2]),
        ]

    for b in range(8):
        for copy in copies(b):
            copy.start()
    sign = signs()
    a = angle[0:1, :]
    for b in range(8):
        if b % GROUP == 0:
            for near_by in range(b, b + GROUP):
                for copy in copies(near_by):
                    copy.wait()
        re, im = turned(held[b, 0], held[b, 1], a * held[b, 2])
        for c, part in enumerate(mixed(re, im, sign)):
            for r, tile in enumerate(walsh(tiles(part))):
                state[b * 2 + c, r * 8 : r * 8 + 8, :] = tile
        for top in range(2):
            for low in range(8):
                out[b * 16 + top * 8 + low, 2] = held[b, 2, pl.ds(top * 64 + low, 8, stride=8), :]
            for c in range(2):
                rows = [state[b * 2 + c, pl.ds(top * 64 + low, 8, stride=8), :] for low in range(8)]
                for low, tile in enumerate(walsh(rows)):
                    out[b * 16 + top * 8 + low, c] = tile
    for r in range(16):
        for c in range(2):
            for b, tile in enumerate(walsh([out[b * 16 + r, c] for b in range(8)])):
                out[b * 16 + r, c] = tile


def second_kernel(got, angle, out):
    sign = signs()
    a = angle[1:2, :]
    upper = lax.broadcasted_iota(jnp.int32, (8, 128), 0) < 4
    for r in range(16):
        for c in range(2):
            for b, tile in enumerate(walsh([got[b * 16 + r, c] * HALF for b in range(8)])):
                out[b * 16 + r, c] = tile
    for b in range(8):
        rows = range(b * 16, b * 16 + 16)
        re = jnp.concatenate(walsh([out[r, 0] for r in rows]), 0)
        im = jnp.concatenate(walsh([out[r, 1] for r in rows]), 0)
        e = got[b * 16 : b * 16 + 16, 2].reshape(128, 128)
        re, im = turned(re, im, a * e)
        for c, part in enumerate(mixed(re, im, sign)):
            mid = walsh(tiles(part))
            for r in range(0, 16, 2):
                u = jnp.where(upper, mid[r], pltpu.roll(mid[r + 1], 4, 0))
                v = jnp.where(upper, pltpu.roll(mid[r], 4, 0), mid[r + 1])
                out[b * 16 + r, c] = u + v
                out[b * 16 + r + 1, c] = u - v
    for r in range(16):
        for c in range(2):
            for b, tile in enumerate(walsh([out[b * 16 + r, c] for b in range(8)])):
                out[b * 16 + r, c] = tile


def third_kernel(place, got, mine, away, keep, send, held, state):
    for r in range(16):
        for c in range(2):
            for b, tile in enumerate(walsh([got[b * 16 + r, c] * HALF for b in range(8)])):
                held[b * 16 + r, c] = tile
    core = (place[0] & 1) == 0
    far = (place[0] >> 1) == 0
    for b in range(8):
        chance = []
        for c in range(2):
            for r, tile in enumerate(walsh([held[b * 16 + r, c] for r in range(16)])):
                state[b * 2 + c, pl.ds(r // 8 * 64 + r % 8, 8, stride=8), :] = tile
            for top in range(2):
                both = []
                for half in range(2):
                    rows = [top * 64 + half * 32 + mid * 8 for mid in range(4)]
                    both.append(walsh([state[b * 2 + c, r : r + 8, :] for r in rows]))
                for mid, (u, v) in enumerate(zip(*both)):
                    mine[c, b, top, mid * 8 : mid * 8 + 8, :] = jnp.where(core, u, v)
                    away[c, b, top, mid * 8 : mid * 8 + 8, :] = jnp.where(core, v, u)
                    chance.append(u * u + v * v)
        for mid in range(4):
            u = (chance[mid] + chance[8 + mid]) * 0.25
            v = (chance[4 + mid] + chance[12 + mid]) * 0.25
            keep[b, mid * 8 : mid * 8 + 8, :] = jnp.where(far, u, v)
            send[b, mid * 8 : mid * 8 + 8, :] = jnp.where(far, v, u)


def last_kernel(place, mine, other, out, done):
    core = place[0] & 1
    copies = []
    for c in range(2):
        copies.append(pltpu.make_async_copy(mine.at[c], out.at[c, :, :, core], done.at[0, c]))
        copies.append(pltpu.make_async_copy(other.at[c], out.at[c, :, :, 1 - core], done.at[1, c]))
    for copy in copies:
        copy.start()
    for copy in copies:
        copy.wait()


def here(*dims):
    return pltpu.VMEM(dims, F32)


def near(x):
    return pltpu.with_memory_space_constraint(x, pltpu.VMEM)


VMEM = pl.BlockSpec(memory_space=pltpu.VMEM)
SMEM = pl.BlockSpec(memory_space=pltpu.SMEM)
HBM = pl.BlockSpec(memory_space=pltpu.HBM)
BOTH = ("bank", "lane")
ORDER = ("lane", "bank")


def shards(amplitudes, energies, diagonal_angles):
    diagonal_angles, bank = lax.optimization_barrier((diagonal_angles, lax.axis_index("bank")))
    values = pl.pallas_call(
        first_kernel,
        out_shape=here(128, 3, 8, 128),
        in_specs=[HBM, HBM, VMEM],
        out_specs=VMEM,
        scratch_shapes=[here(8, 3, 128, 128), here(16, 128, 128), pltpu.SemaphoreType.DMA((8, 3))],
        name="first",
    )(amplitudes, energies, diagonal_angles)
    values = lax.all_to_all(values.reshape(128, 24, 128), ORDER, 0, 0, tiled=True)
    values = pl.pallas_call(
        second_kernel, out_shape=here(128, 2, 8, 128), in_specs=[VMEM] * 2, out_specs=VMEM, name="second"
    )(near(values.reshape(128, 3, 8, 128)), diagonal_angles)
    values = lax.all_to_all(values.reshape(128, 16, 128), ORDER, 0, 0, tiled=True)
    place = bank.reshape(1)
    mine, away, keep, send = pl.pallas_call(
        third_kernel,
        out_shape=(here(2, 8, 2, 32, 128), here(2, 8, 2, 32, 128), here(8, 32, 128), here(8, 32, 128)),
        in_specs=[SMEM, VMEM],
        out_specs=(VMEM,) * 4,
        scratch_shapes=[here(128, 2, 8, 128), here(16, 128, 128)],
        name="third",
    )(place, near(values.reshape(128, 2, 8, 128)))
    other = lax.ppermute(away, "bank", [(i, i ^ 1) for i in range(4)])
    final = pl.pallas_call(
        last_kernel,
        out_shape=jax.ShapeDtypeStruct((2, 8, 2, 2, 32, 128), F32),
        in_specs=[SMEM, VMEM, VMEM],
        out_specs=HBM,
        scratch_shapes=[pltpu.SemaphoreType.DMA((2, 2))],
        name="last",
    )(place, near(mine), near(other))
    sent = lax.ppermute(send, "bank", [(i, i ^ 2) for i in range(4)])
    marginal = keep + sent
    return final.reshape(2, 8, 128, 128), marginal


def solution(mesh):
    return jax.shard_map(
        shards,
        mesh=mesh,
        in_specs=(P(None, BOTH, None, None), P(BOTH, None, None), P()),
        out_specs=(P(None, BOTH, None, None), P("lane", "bank", None)),
        check_vma=False,
    )
```

```python
import jax
import jax.numpy as jnp
import numpy as np
from jax import lax
from jax.experimental import pallas as pl
from jax.experimental.pallas import tpu as pltpu
from jax.sharding import PartitionSpec as P


F32 = jnp.float32
BF16 = jnp.bfloat16
GROUPS = (2, 3, 3)
SCALE = 2.0**-13


def fit(terms, reach):
    k = np.arange(400)
    x = reach * np.cos(np.pi * (k + 0.5) / 400)
    powers = np.stack([x ** (2 * n + 1) for n in range(terms)], 1)
    scale = np.abs(powers).max(0)
    return [float(c) for c in np.linalg.lstsq(powers / scale, 2 * np.sin(x), rcond=None)[0] / scale]


SIN = fit(6, 1.4)


def turned(re, im, half):
    square = half * half
    sin = jnp.full_like(half, SIN[-1])
    for c in SIN[-2::-1]:
        sin = sin * square + c
    sin = sin * half
    square = sin * sin
    rest = 4.0 - square
    cos, sin = 2.0 - square, sin * (rest * lax.rsqrt(rest))
    return re * cos + im * sin, im * cos - re * sin


def walsh(parts):
    parts, step = list(parts), 1
    while step < len(parts):
        for i in range(len(parts)):
            if not i & step:
                u, v = parts[i], parts[i + step]
                parts[i], parts[i + step] = u + v, u - v
        step *= 2
    return parts


def signs():
    both = lax.broadcasted_iota(jnp.int32, (128, 128), 0) & lax.broadcasted_iota(jnp.int32, (128, 128), 1)
    for shift in (4, 2, 1):
        both = both ^ (both >> shift)
    return ((1 - 2 * (both & 1)).astype(F32) * SCALE).astype(BF16)


PIECES = 2


def mixed(re, im, sign):
    rest = jnp.concatenate([re, im], 0)
    pieces = []
    for _ in range(PIECES):
        pieces.append(rest.astype(BF16))
        rest = rest - pieces[-1].astype(F32)
    both = jnp.dot(jnp.concatenate(pieces, 1), jnp.concatenate([sign] * PIECES, 0), preferred_element_type=F32)
    return both[:128], both[128:]


def tiles(x):
    return [x[r * 8 : r * 8 + 8] for r in range(x.shape[0] // 8)]


def first_kernel(amp, ener, angle, out, held, state, arrived):
    def copies(b):
        return [
            pltpu.make_async_copy(amp.at[0, b], held.at[b, 0], arrived.at[b, 0]),
            pltpu.make_async_copy(amp.at[1, b], held.at[b, 1], arrived.at[b, 1]),
            pltpu.make_async_copy(ener.at[b], held.at[b, 2], arrived.at[b, 2]),
        ]

    for b in range(8):
        for copy in copies(b):
            copy.start()
    starts = {sum(GROUPS[:i]): size for i, size in enumerate(GROUPS)}
    sign = signs()
    a = angle[0:1, :] * 0.5
    for b in range(8):
        if b in starts:
            for ready in range(b, b + starts[b]):
                for copy in copies(ready):
                    copy.wait()
        re, im = turned(held[b, 0], held[b, 1], a * held[b, 2])
        for c, part in enumerate(mixed(re, im, sign)):
            for r, tile in enumerate(walsh(tiles(part))):
                state[b * 2 + c, r * 8 : r * 8 + 8, :] = tile
        for top in range(2):
            for low in range(8):
                out[b * 16 + top * 8 + low, 2] = held[b, 2, pl.ds(top * 64 + low, 8, stride=8), :]
            for c in range(2):
                rows = [state[b * 2 + c, pl.ds(top * 64 + low, 8, stride=8), :] for low in range(8)]
                for low, tile in enumerate(walsh(rows)):
                    out[b * 16 + top * 8 + low, c] = tile
    for r in range(16):
        for c in range(2):
            for b, tile in enumerate(walsh([out[b * 16 + r, c] for b in range(8)])):
                out[b * 16 + r, c] = tile


def second_kernel(got, angle, out):
    sign = signs()
    a = angle[1:2, :] * 0.5
    upper = lax.broadcasted_iota(jnp.int32, (8, 128), 0) < 4
    for r in range(16):
        for c in range(2):
            for b, tile in enumerate(walsh([got[b * 16 + r, c] for b in range(8)])):
                out[b * 16 + r, c] = tile
    for b in range(8):
        rows = range(b * 16, b * 16 + 16)
        re = jnp.concatenate(walsh([out[r, 0] for r in rows]), 0)
        im = jnp.concatenate(walsh([out[r, 1] for r in rows]), 0)
        e = got[b * 16 : b * 16 + 16, 2].reshape(128, 128)
        re, im = turned(re, im, a * e)
        for c, part in enumerate(mixed(re, im, sign)):
            mid = walsh(tiles(part))
            for r in range(0, 16, 2):
                u = jnp.where(upper, mid[r], pltpu.roll(mid[r + 1], 4, 0))
                v = jnp.where(upper, pltpu.roll(mid[r], 4, 0), mid[r + 1])
                out[b * 16 + r, c] = u + v
                out[b * 16 + r + 1, c] = u - v
    for r in range(16):
        for c in range(2):
            for b, tile in enumerate(walsh([out[b * 16 + r, c] for b in range(8)])):
                out[b * 16 + r, c] = tile


def third_kernel(place, got, mine, away, keep, send, held, state):
    for r in range(16):
        for c in range(2):
            for b, tile in enumerate(walsh([got[b * 16 + r, c] for b in range(8)])):
                held[b * 16 + r, c] = tile
    core = (place[0] & 1) == 0
    far = (place[0] >> 1) == 0
    for b in range(8):
        chance = []
        for c in range(2):
            for r, tile in enumerate(walsh([held[b * 16 + r, c] for r in range(16)])):
                state[b * 2 + c, pl.ds(r // 8 * 64 + r % 8, 8, stride=8), :] = tile
            for top in range(2):
                both = []
                for half in range(2):
                    rows = [top * 64 + half * 32 + mid * 8 for mid in range(4)]
                    both.append(walsh([state[b * 2 + c, r : r + 8, :] for r in rows]))
                for mid, (u, v) in enumerate(zip(*both)):
                    mine[c, b, top, mid * 8 : mid * 8 + 8, :] = jnp.where(core, u, v)
                    away[c, b, top, mid * 8 : mid * 8 + 8, :] = jnp.where(core, v, u)
                    chance.append(u * u + v * v)
        for mid in range(4):
            u = (chance[mid] + chance[8 + mid]) * 0.25
            v = (chance[4 + mid] + chance[12 + mid]) * 0.25
            keep[b, mid * 8 : mid * 8 + 8, :] = jnp.where(far, u, v)
            send[b, mid * 8 : mid * 8 + 8, :] = jnp.where(far, v, u)


def last_kernel(place, mine, other, out, done):
    core = place[0] & 1
    copies = []
    for c in range(2):
        copies.append(pltpu.make_async_copy(mine.at[c], out.at[c, :, :, core], done.at[0, c]))
        copies.append(pltpu.make_async_copy(other.at[c], out.at[c, :, :, 1 - core], done.at[1, c]))
    for copy in copies:
        copy.start()
    for copy in copies:
        copy.wait()


def here(*dims):
    return pltpu.VMEM(dims, F32)


def near(x):
    return pltpu.with_memory_space_constraint(x, pltpu.VMEM)


VMEM = pl.BlockSpec(memory_space=pltpu.VMEM)
SMEM = pl.BlockSpec(memory_space=pltpu.SMEM)
HBM = pl.BlockSpec(memory_space=pltpu.HBM)
BOTH = ("bank", "lane")
ORDER = ("lane", "bank")


def shards(amplitudes, energies, diagonal_angles):
    diagonal_angles, bank = lax.optimization_barrier((diagonal_angles, lax.axis_index("bank")))
    values = pl.pallas_call(
        first_kernel,
        out_shape=here(128, 3, 8, 128),
        in_specs=[HBM, HBM, VMEM],
        out_specs=VMEM,
        scratch_shapes=[here(8, 3, 128, 128), here(16, 128, 128), pltpu.SemaphoreType.DMA((8, 3))],
        name="first",
    )(amplitudes, energies, diagonal_angles)
    values = lax.all_to_all(values.reshape(128, 24, 128), ORDER, 0, 0, tiled=True)
    values = pl.pallas_call(
        second_kernel, out_shape=here(128, 2, 8, 128), in_specs=[VMEM] * 2, out_specs=VMEM, name="second"
    )(near(values.reshape(128, 3, 8, 128)), diagonal_angles)
    values = lax.all_to_all(values.reshape(128, 16, 128), ORDER, 0, 0, tiled=True)
    place = bank.reshape(1)
    mine, away, keep, send = pl.pallas_call(
        third_kernel,
        out_shape=(here(2, 8, 2, 32, 128), here(2, 8, 2, 32, 128), here(8, 32, 128), here(8, 32, 128)),
        in_specs=[SMEM, VMEM],
        out_specs=(VMEM,) * 4,
        scratch_shapes=[here(128, 2, 8, 128), here(16, 128, 128)],
        name="third",
    )(place, near(values.reshape(128, 2, 8, 128)))
    other = lax.ppermute(away, "bank", [(i, i ^ 1) for i in range(4)])
    final = pl.pallas_call(
        last_kernel,
        out_shape=jax.ShapeDtypeStruct((2, 8, 2, 2, 32, 128), F32),
        in_specs=[SMEM, VMEM, VMEM],
        out_specs=HBM,
        scratch_shapes=[pltpu.SemaphoreType.DMA((2, 2))],
        name="last",
    )(place, near(mine), near(other))
    sent = lax.ppermute(send, "bank", [(i, i ^ 2) for i in range(4)])
    marginal = keep + sent
    return final.reshape(2, 8, 128, 128), marginal


def solution(mesh):
    return jax.shard_map(
        shards,
        mesh=mesh,
        in_specs=(P(None, BOTH, None, None), P(BOTH, None, None), P()),
        out_specs=(P(None, BOTH, None, None), P("lane", "bank", None)),
        check_vma=False,
    )
```

```python
import jax
import jax.numpy as jnp
import numpy as np
from jax import lax
from jax.experimental import pallas as pl
from jax.experimental.pallas import tpu as pltpu
from jax.sharding import Mesh, PartitionSpec as P


F32 = jnp.float32
BF16 = jnp.bfloat16
GROUPS = (2, 3, 3)
SCALE = 2.0**-13


def fit(terms, reach):
    k = np.arange(400)
    x = reach * np.cos(np.pi * (k + 0.5) / 400)
    powers = np.stack([x ** (2 * n + 1) for n in range(terms)], 1)
    scale = np.abs(powers).max(0)
    return [float(c) for c in np.linalg.lstsq(powers / scale, 2 * np.sin(x), rcond=None)[0] / scale]


SIN = fit(6, 1.4)


def turned(re, im, half):
    square = half * half
    sin = jnp.full_like(half, SIN[-1])
    for c in SIN[-2::-1]:
        sin = sin * square + c
    sin = sin * half
    square = sin * sin
    rest = 4.0 - square
    cos, sin = 2.0 - square, sin * (rest * lax.rsqrt(rest))
    return re * cos + im * sin, im * cos - re * sin


def walsh(parts):
    parts, step = list(parts), 1
    while step < len(parts):
        for i in range(len(parts)):
            if not i & step:
                u, v = parts[i], parts[i + step]
                parts[i], parts[i + step] = u + v, u - v
        step *= 2
    return parts


def signs():
    both = lax.broadcasted_iota(jnp.int32, (128, 128), 0) & lax.broadcasted_iota(jnp.int32, (128, 128), 1)
    for shift in (4, 2, 1):
        both = both ^ (both >> shift)
    return ((1 - 2 * (both & 1)).astype(F32) * SCALE).astype(BF16)


PIECES = 2


def mixed(re, im, sign):
    rest = jnp.concatenate([re, im], 0)
    pieces = []
    for _ in range(PIECES):
        pieces.append(rest.astype(BF16))
        rest = rest - pieces[-1].astype(F32)
    both = jnp.dot(jnp.concatenate(pieces, 1), jnp.concatenate([sign] * PIECES, 0), preferred_element_type=F32)
    return both[:128], both[128:]


def tiles(x):
    return [x[r * 8 : r * 8 + 8] for r in range(x.shape[0] // 8)]


def first_kernel(amp, ener, angle, out, held, state, arrived):
    def copies(b):
        return [
            pltpu.make_async_copy(amp.at[0, b], held.at[b, 0], arrived.at[b, 0]),
            pltpu.make_async_copy(amp.at[1, b], held.at[b, 1], arrived.at[b, 1]),
            pltpu.make_async_copy(ener.at[b], held.at[b, 2], arrived.at[b, 2]),
        ]

    for b in range(8):
        for copy in copies(b):
            copy.start()
    starts = {sum(GROUPS[:i]): size for i, size in enumerate(GROUPS)}
    sign = signs()
    a = angle[0:1, :] * 0.5
    for b in range(8):
        if b in starts:
            for ready in range(b, b + starts[b]):
                for copy in copies(ready):
                    copy.wait()
        re, im = turned(held[b, 0], held[b, 1], a * held[b, 2])
        for c, part in enumerate(mixed(re, im, sign)):
            for r, tile in enumerate(walsh(tiles(part))):
                state[b * 2 + c, r * 8 : r * 8 + 8, :] = tile
        for top in range(2):
            for low in range(8):
                out[b * 16 + top * 8 + low, 2] = held[b, 2, pl.ds(top * 64 + low, 8, stride=8), :]
            for c in range(2):
                rows = [state[b * 2 + c, pl.ds(top * 64 + low, 8, stride=8), :] for low in range(8)]
                for low, tile in enumerate(walsh(rows)):
                    out[b * 16 + top * 8 + low, c] = tile
    for r in range(16):
        for c in range(2):
            for b, tile in enumerate(walsh([out[b * 16 + r, c] for b in range(8)])):
                out[b * 16 + r, c] = tile


def second_kernel(got, angle, out, held, state):
    sign = signs()
    a = angle[1:2, :] * 0.5
    for r in range(16):
        rows = [r // 8 * 64 + high * 8 + r % 8 for high in range(8)]
        for c in range(2):
            for row, tile in zip(rows, walsh([got[row, c] for row in rows])):
                held[row, c] = tile
    for high in range(8):
        rows = [core * 64 + high * 8 + low for core in range(2) for low in range(8)]
        re = jnp.concatenate(walsh([held[row, 0] for row in rows]), 0)
        im = jnp.concatenate(walsh([held[row, 1] for row in rows]), 0)
        e = jnp.concatenate([got[row, 2] for row in rows], 0)
        re, im = turned(re, im, a * e)
        for c, part in enumerate(mixed(re, im, sign)):
            for r, tile in enumerate(walsh(tiles(part))):
                state[c, high * 8 + r % 8, pl.ds(r // 8, 8, stride=2), :] = tile
    for low in range(8):
        for c in range(2):
            parts = [state[c, high * 8 + low, r5 * 8 : r5 * 8 + 8, :] for r5 in range(2) for high in range(8)]
            for r, tile in enumerate(walsh(parts)):
                out[r // 8 * 64 + r % 8 * 8 + low, c] = tile


def third_kernel(place, got, mine, away, keep, send, held, state):
    for r in range(16):
        for c in range(2):
            for b, tile in enumerate(walsh([got[b * 16 + r, c] for b in range(8)])):
                held[b * 16 + r, c] = tile
    core = (place[0] & 1) == 0
    far = (place[0] >> 1) == 0
    for b in range(8):
        chance = []
        for c in range(2):
            for r, tile in enumerate(walsh([held[b * 16 + r, c] for r in range(16)])):
                state[b * 2 + c, pl.ds(r // 8 * 64 + r % 8, 8, stride=8), :] = tile
            for top in range(2):
                both = []
                for half in range(2):
                    rows = [top * 64 + mid * 16 + half * 8 for mid in range(4)]
                    both.append(walsh([state[b * 2 + c, r : r + 8, :] for r in rows]))
                for mid, (u, v) in enumerate(zip(*both)):
                    mine[c, b, top, mid * 8 : mid * 8 + 8, :] = jnp.where(core, u, v)
                    away[c, b, top, mid * 8 : mid * 8 + 8, :] = jnp.where(core, v, u)
                    chance.append(u * u + v * v)
        for mid in range(4):
            u = (chance[mid] + chance[8 + mid]) * 0.25
            v = (chance[4 + mid] + chance[12 + mid]) * 0.25
            keep[b, mid * 8 : mid * 8 + 8, :] = jnp.where(far, u, v)
            send[b, mid * 8 : mid * 8 + 8, :] = jnp.where(far, v, u)


def last_kernel(place, mine, other, out, done):
    core = place[0] & 1
    copies = []
    for c in range(2):
        copies.append(pltpu.make_async_copy(mine.at[c], out.at[c, :, :, core], done.at[0, c]))
        copies.append(pltpu.make_async_copy(other.at[c], out.at[c, :, :, 1 - core], done.at[1, c]))
    for copy in copies:
        copy.start()
    for copy in copies:
        copy.wait()


def here(*dims):
    return pltpu.VMEM(dims, F32)


def near(x):
    return pltpu.with_memory_space_constraint(x, pltpu.VMEM)


VMEM = pl.BlockSpec(memory_space=pltpu.VMEM)
SMEM = pl.BlockSpec(memory_space=pltpu.SMEM)
HBM = pl.BlockSpec(memory_space=pltpu.HBM)
BANK = ("x_hi", "core")
LANE = ("z", "y", "x_lo")
ORDER = ("core", "y", "x_hi", "x_lo", "z")


def shards(amplitudes, energies, diagonal_angles):
    diagonal_angles, bank = lax.optimization_barrier((diagonal_angles, lax.axis_index(BANK)))
    values = pl.pallas_call(
        first_kernel,
        out_shape=here(128, 3, 8, 128),
        in_specs=[HBM, HBM, VMEM],
        out_specs=VMEM,
        scratch_shapes=[here(8, 3, 128, 128), here(16, 128, 128), pltpu.SemaphoreType.DMA((8, 3))],
        name="first",
    )(amplitudes, energies, diagonal_angles)
    values = lax.all_to_all(values.reshape(128, 24, 128), ORDER, 0, 0, tiled=True)
    values = pl.pallas_call(
        second_kernel,
        out_shape=here(128, 2, 8, 128),
        in_specs=[VMEM] * 2,
        out_specs=VMEM,
        scratch_shapes=[here(128, 2, 8, 128), here(2, 64, 16, 128)],
        name="second",
    )(near(values.reshape(128, 3, 8, 128)), diagonal_angles)
    values = lax.all_to_all(values.reshape(128, 16, 128), ORDER, 0, 0, tiled=True)
    place = bank.reshape(1)
    mine, away, keep, send = pl.pallas_call(
        third_kernel,
        out_shape=(here(2, 8, 2, 32, 128), here(2, 8, 2, 32, 128), here(8, 32, 128), here(8, 32, 128)),
        in_specs=[SMEM, VMEM],
        out_specs=(VMEM,) * 4,
        scratch_shapes=[here(128, 2, 8, 128), here(16, 128, 128)],
        name="third",
    )(place, near(values.reshape(128, 2, 8, 128)))
    other = lax.ppermute(away, "core", [(0, 1), (1, 0)])
    final = pl.pallas_call(
        last_kernel,
        out_shape=jax.ShapeDtypeStruct((2, 8, 2, 2, 32, 128), F32),
        in_specs=[SMEM, VMEM, VMEM],
        out_specs=HBM,
        scratch_shapes=[pltpu.SemaphoreType.DMA((2, 2))],
        name="last",
    )(place, near(mine), near(other))
    sent = lax.ppermute(send, "x_hi", [(0, 1), (1, 0)])
    marginal = keep + sent
    return final.reshape(2, 8, 128, 128), marginal


def solution(mesh):
    mesh = Mesh(mesh.devices.reshape(2, 2, 4, 4, 2), BANK + LANE)
    return jax.shard_map(
        shards,
        mesh=mesh,
        in_specs=(P(None, BANK + LANE, None, None), P(BANK + LANE, None, None), P()),
        out_specs=(P(None, BANK + LANE, None, None), P(LANE, BANK, None)),
        check_vma=False,
    )
```

```python
import jax
import jax.numpy as jnp
import numpy as np
from jax import lax
from jax.experimental import pallas as pl
from jax.experimental.pallas import tpu as pltpu
from jax.sharding import Mesh, PartitionSpec as P


F32 = jnp.float32
BF16 = jnp.bfloat16
GROUPS = (2, 3, 3)
SCALE = 2.0**-13


def fit(terms, reach):
    k = np.arange(400)
    x = reach * np.cos(np.pi * (k + 0.5) / 400)
    powers = np.stack([x ** (2 * n + 1) for n in range(terms)], 1)
    scale = np.abs(powers).max(0)
    return [float(c) for c in np.linalg.lstsq(powers / scale, 2 * np.sin(x), rcond=None)[0] / scale]


SIN = fit(6, 1.4)


def turned(re, im, half):
    square = half * half
    sin = jnp.full_like(half, SIN[-1])
    for c in SIN[-2::-1]:
        sin = sin * square + c
    sin = sin * half
    square = sin * sin
    rest = 4.0 - square
    cos, sin = 2.0 - square, sin * (rest * lax.rsqrt(rest))
    return re * cos + im * sin, im * cos - re * sin


def walsh(parts):
    parts, step = list(parts), 1
    while step < len(parts):
        for i in range(len(parts)):
            if not i & step:
                u, v = parts[i], parts[i + step]
                parts[i], parts[i + step] = u + v, u - v
        step *= 2
    return parts


def signs():
    both = lax.broadcasted_iota(jnp.int32, (128, 128), 0) & lax.broadcasted_iota(jnp.int32, (128, 128), 1)
    for shift in (4, 2, 1):
        both = both ^ (both >> shift)
    return ((1 - 2 * (both & 1)).astype(F32) * SCALE).astype(BF16)


PIECES = 2


def mixed(re, im, sign):
    rest = jnp.concatenate([re, im], 0)
    pieces = []
    for _ in range(PIECES):
        pieces.append(rest.astype(BF16))
        rest = rest - pieces[-1].astype(F32)
    both = jnp.dot(jnp.concatenate(pieces, 1), jnp.concatenate([sign] * PIECES, 0), preferred_element_type=F32)
    return both[:128], both[128:]


def tiles(x):
    return [x[r * 8 : r * 8 + 8] for r in range(x.shape[0] // 8)]


def first_kernel(amp, ener, angle, out, held, state, arrived):
    def copies(b):
        return [
            pltpu.make_async_copy(amp.at[0, b], held.at[b, 0], arrived.at[b, 0]),
            pltpu.make_async_copy(amp.at[1, b], held.at[b, 1], arrived.at[b, 1]),
            pltpu.make_async_copy(ener.at[b], held.at[b, 2], arrived.at[b, 2]),
        ]

    for b in range(8):
        for copy in copies(b):
            copy.start()
    starts = {sum(GROUPS[:i]): size for i, size in enumerate(GROUPS)}
    sign = signs()
    a = angle[0:1, :] * 0.5
    for b in range(8):
        if b in starts:
            for ready in range(b, b + starts[b]):
                for copy in copies(ready):
                    copy.wait()
        re, im = turned(held[b, 0], held[b, 1], a * held[b, 2])
        for c, part in enumerate(mixed(re, im, sign)):
            for r, tile in enumerate(walsh(tiles(part))):
                state[b * 2 + c, r * 8 : r * 8 + 8, :] = tile
        for top in range(2):
            for low in range(8):
                out[b * 16 + top * 8 + low, 2] = held[b, 2, pl.ds(top * 64 + low, 8, stride=8), :]
            for c in range(2):
                rows = [state[b * 2 + c, pl.ds(top * 64 + low, 8, stride=8), :] for low in range(8)]
                for low, tile in enumerate(walsh(rows)):
                    out[b * 16 + top * 8 + low, c] = tile
    for r in range(16):
        for c in range(2):
            for b, tile in enumerate(walsh([out[b * 16 + r, c] for b in range(8)])):
                out[b * 16 + r, c] = tile


def second_kernel(got, angle, out, held, state):
    sign = signs()
    a = angle[1:2, :] * 0.5
    for r in range(16):
        rows = [r // 8 * 64 + high * 8 + r % 8 for high in range(8)]
        for c in range(2):
            for row, tile in zip(rows, walsh([got[row, c] for row in rows])):
                held[row, c] = tile
    for high in range(8):
        rows = [core * 64 + high * 8 + low for core in range(2) for low in range(8)]
        re = jnp.concatenate(walsh([held[row, 0] for row in rows]), 0)
        im = jnp.concatenate(walsh([held[row, 1] for row in rows]), 0)
        e = jnp.concatenate([got[row, 2] for row in rows], 0)
        re, im = turned(re, im, a * e)
        for c, part in enumerate(mixed(re, im, sign)):
            for r, tile in enumerate(walsh(tiles(part))):
                state[c, high * 8 + r % 8, pl.ds(r // 8, 8, stride=2), :] = tile
    for low in range(8):
        for c in range(2):
            parts = [state[c, high * 8 + low, r5 * 8 : r5 * 8 + 8, :] for r5 in range(2) for high in range(8)]
            for r, tile in enumerate(walsh(parts)):
                out[r // 8 * 64 + r % 8 * 8 + low, c] = tile


def third_kernel(place, got, send, held, state):
    side = jnp.full((8, 128), (2 * (place[0] >> 1) - 1).astype(F32))
    for r in range(16):
        for c in range(2):
            for b, tile in enumerate(walsh([got[b * 16 + r, c] for b in range(8)])):
                held[b * 16 + r, c] = tile
    for b in range(8):
        chance = [0.0] * 4
        for c in range(2):
            low = [held[b * 16 + r, c] + side * held[b * 16 + 8 + r, c] for r in range(8)]
            for r, tile in enumerate(walsh(low)):
                state[b * 2 + c, pl.ds(r, 8, stride=8), :] = tile
            for half in range(2):
                rows = [mid * 16 + half * 8 for mid in range(4)]
                for mid, u in enumerate(walsh([state[b * 2 + c, r : r + 8, :] for r in rows])):
                    chance[mid] = chance[mid] + u * u
        for mid in range(4):
            send[b, mid * 8 : mid * 8 + 8, :] = chance[mid] * 0.25


def fourth_kernel(place, held, mine, away, keep, state):
    core = (place[0] & 1) == 0
    far = (place[0] >> 1) == 0
    for b in range(8):
        chance = []
        for c in range(2):
            for r, tile in enumerate(walsh([held[b * 16 + r, c] for r in range(16)])):
                state[b * 2 + c, pl.ds(r // 8 * 64 + r % 8, 8, stride=8), :] = tile
            for top in range(2):
                both = []
                for half in range(2):
                    rows = [top * 64 + mid * 16 + half * 8 for mid in range(4)]
                    both.append(walsh([state[b * 2 + c, r : r + 8, :] for r in rows]))
                for mid, (u, v) in enumerate(zip(*both)):
                    mine[c, b, top, mid * 8 : mid * 8 + 8, :] = jnp.where(core, u, v)
                    away[c, b, top, mid * 8 : mid * 8 + 8, :] = jnp.where(core, v, u)
                    chance.append(u * u + v * v)
        for mid in range(4):
            u = (chance[mid] + chance[8 + mid]) * 0.25
            v = (chance[4 + mid] + chance[12 + mid]) * 0.25
            keep[b, mid * 8 : mid * 8 + 8, :] = jnp.where(far, u, v)


def last_kernel(place, mine, other, out, done):
    core = place[0] & 1
    copies = []
    for c in range(2):
        copies.append(pltpu.make_async_copy(mine.at[c], out.at[c, :, :, core], done.at[0, c]))
        copies.append(pltpu.make_async_copy(other.at[c], out.at[c, :, :, 1 - core], done.at[1, c]))
    for copy in copies:
        copy.start()
    for copy in copies:
        copy.wait()


def here(*dims):
    return pltpu.VMEM(dims, F32)


def near(x):
    return pltpu.with_memory_space_constraint(x, pltpu.VMEM)


VMEM = pl.BlockSpec(memory_space=pltpu.VMEM)
SMEM = pl.BlockSpec(memory_space=pltpu.SMEM)
HBM = pl.BlockSpec(memory_space=pltpu.HBM)
BANK = ("x_hi", "core")
LANE = ("z", "y", "x_lo")
ORDER = ("core", "y", "x_hi", "x_lo", "z")


def shards(amplitudes, energies, diagonal_angles):
    diagonal_angles, bank = lax.optimization_barrier((diagonal_angles, lax.axis_index(BANK)))
    values = pl.pallas_call(
        first_kernel,
        out_shape=here(128, 3, 8, 128),
        in_specs=[HBM, HBM, VMEM],
        out_specs=VMEM,
        scratch_shapes=[here(8, 3, 128, 128), here(16, 128, 128), pltpu.SemaphoreType.DMA((8, 3))],
        name="first",
    )(amplitudes, energies, diagonal_angles)
    values = lax.all_to_all(values.reshape(128, 24, 128), ORDER, 0, 0, tiled=True)
    values = pl.pallas_call(
        second_kernel,
        out_shape=here(128, 2, 8, 128),
        in_specs=[VMEM] * 2,
        out_specs=VMEM,
        scratch_shapes=[here(128, 2, 8, 128), here(2, 64, 16, 128)],
        name="second",
    )(near(values.reshape(128, 3, 8, 128)), diagonal_angles)
    values = lax.all_to_all(values.reshape(128, 16, 128), ORDER, 0, 0, tiled=True)
    place = bank.reshape(1)
    send, held = pl.pallas_call(
        third_kernel,
        out_shape=(here(8, 32, 128), here(128, 2, 8, 128)),
        in_specs=[SMEM, VMEM],
        out_specs=(VMEM, VMEM),
        scratch_shapes=[here(16, 64, 128)],
        name="third",
    )(place, near(values.reshape(128, 2, 8, 128)))
    sent = lax.ppermute(send, "x_hi", [(0, 1), (1, 0)])
    mine, away, keep = pl.pallas_call(
        fourth_kernel,
        out_shape=(here(2, 8, 2, 32, 128), here(2, 8, 2, 32, 128), here(8, 32, 128)),
        in_specs=[SMEM, VMEM],
        out_specs=(VMEM,) * 3,
        scratch_shapes=[here(16, 128, 128)],
        name="fourth",
    )(place, near(held))
    other = lax.ppermute(away, "core", [(0, 1), (1, 0)])
    final = pl.pallas_call(
        last_kernel,
        out_shape=jax.ShapeDtypeStruct((2, 8, 2, 2, 32, 128), F32),
        in_specs=[SMEM, VMEM, VMEM],
        out_specs=HBM,
        scratch_shapes=[pltpu.SemaphoreType.DMA((2, 2))],
        name="last",
    )(place, near(mine), near(other))
    marginal = keep + sent
    return final.reshape(2, 8, 128, 128), marginal


def solution(mesh):
    mesh = Mesh(mesh.devices.reshape(2, 2, 4, 4, 2), BANK + LANE)
    return jax.shard_map(
        shards,
        mesh=mesh,
        in_specs=(P(None, BANK + LANE, None, None), P(BANK + LANE, None, None), P()),
        out_specs=(P(None, BANK + LANE, None, None), P(LANE, BANK, None)),
        check_vma=False,
    )
```

```python
import jax
import jax.numpy as jnp
import numpy as np
from jax import lax
from jax.experimental import pallas as pl
from jax.experimental.pallas import tpu as pltpu
from jax.sharding import Mesh, PartitionSpec as P


F32 = jnp.float32
BF16 = jnp.bfloat16
GROUPS = (2, 3, 3)
SCALE = 2.0**-13


def fit(terms, reach):
    k = np.arange(400)
    x = reach * np.cos(np.pi * (k + 0.5) / 400)
    powers = np.stack([x ** (2 * n + 1) for n in range(terms)], 1)
    scale = np.abs(powers).max(0)
    return [float(c) for c in np.linalg.lstsq(powers / scale, 2 * np.sin(x), rcond=None)[0] / scale]


SIN = fit(6, 1.4)


def turned(re, im, half):
    square = half * half
    sin = jnp.full_like(half, SIN[-1])
    for c in SIN[-2::-1]:
        sin = sin * square + c
    sin = sin * half
    square = sin * sin
    rest = 4.0 - square
    cos, sin = 2.0 - square, sin * (rest * lax.rsqrt(rest))
    return re * cos + im * sin, im * cos - re * sin


def walsh(parts):
    parts, step = list(parts), 1
    while step < len(parts):
        for i in range(len(parts)):
            if not i & step:
                u, v = parts[i], parts[i + step]
                parts[i], parts[i + step] = u + v, u - v
        step *= 2
    return parts


def signs():
    both = lax.broadcasted_iota(jnp.int32, (128, 128), 0) & lax.broadcasted_iota(jnp.int32, (128, 128), 1)
    for shift in (4, 2, 1):
        both = both ^ (both >> shift)
    return ((1 - 2 * (both & 1)).astype(F32) * SCALE).astype(BF16)


PIECES = 2


def mixed(re, im, sign):
    rest = jnp.concatenate([re, im], 0)
    pieces = []
    for _ in range(PIECES):
        pieces.append(rest.astype(BF16))
        rest = rest - pieces[-1].astype(F32)
    both = jnp.dot(jnp.concatenate(pieces, 1), jnp.concatenate([sign] * PIECES, 0), preferred_element_type=F32)
    return both[:128], both[128:]


def tiles(x):
    return [x[r * 8 : r * 8 + 8] for r in range(x.shape[0] // 8)]


def first_kernel(amp, ener, given, out, angle, held, state, arrived, known):
    def copies(b):
        return [
            pltpu.make_async_copy(amp.at[0, b], held.at[b, 0], arrived.at[b, 0]),
            pltpu.make_async_copy(amp.at[1, b], held.at[b, 1], arrived.at[b, 1]),
            pltpu.make_async_copy(ener.at[b], held.at[b, 2], arrived.at[b, 2]),
        ]

    angles = pltpu.make_async_copy(given, angle, known)
    angles.start()
    for b in range(8):
        for copy in copies(b):
            copy.start()
    starts = {sum(GROUPS[:i]): size for i, size in enumerate(GROUPS)}
    sign = signs()
    angles.wait()
    a = angle[0:1, :] * 0.5
    for b in range(8):
        if b in starts:
            for ready in range(b, b + starts[b]):
                for copy in copies(ready):
                    copy.wait()
        re, im = turned(held[b, 0], held[b, 1], a * held[b, 2])
        for c, part in enumerate(mixed(re, im, sign)):
            for r, tile in enumerate(walsh(tiles(part))):
                state[b * 2 + c, r * 8 : r * 8 + 8, :] = tile
        for top in range(2):
            for low in range(8):
                out[b * 16 + top * 8 + low, 2] = held[b, 2, pl.ds(top * 64 + low, 8, stride=8), :]
            for c in range(2):
                rows = [state[b * 2 + c, pl.ds(top * 64 + low, 8, stride=8), :] for low in range(8)]
                for low, tile in enumerate(walsh(rows)):
                    out[b * 16 + top * 8 + low, c] = tile
    for r in range(16):
        for c in range(2):
            for b, tile in enumerate(walsh([out[b * 16 + r, c] for b in range(8)])):
                out[b * 16 + r, c] = tile


def second_kernel(got, angle, out, held, state):
    sign = signs()
    a = angle[1:2, :] * 0.5
    for r in range(16):
        rows = [r // 8 * 64 + high * 8 + r % 8 for high in range(8)]
        for c in range(2):
            for row, tile in zip(rows, walsh([got[row, c] for row in rows])):
                held[row, c] = tile
    for high in range(8):
        rows = [core * 64 + high * 8 + low for core in range(2) for low in range(8)]
        re = jnp.concatenate(walsh([held[row, 0] for row in rows]), 0)
        im = jnp.concatenate(walsh([held[row, 1] for row in rows]), 0)
        e = jnp.concatenate([got[row, 2] for row in rows], 0)
        re, im = turned(re, im, a * e)
        for c, part in enumerate(mixed(re, im, sign)):
            for r, tile in enumerate(walsh(tiles(part))):
                state[c, high * 8 + r % 8, pl.ds(r // 8, 8, stride=2), :] = tile
    for low in range(8):
        for c in range(2):
            parts = [state[c, high * 8 + low, r5 * 8 : r5 * 8 + 8, :] for r5 in range(2) for high in range(8)]
            for r, tile in enumerate(walsh(parts)):
                out[r // 8 * 64 + r % 8 * 8 + low, c] = tile


def third_kernel(place, got, send, held, state):
    side = jnp.full((8, 128), (2 * (place[0] >> 1) - 1).astype(F32))
    for r in range(16):
        for c in range(2):
            for b, tile in enumerate(walsh([got[b * 16 + r, c] for b in range(8)])):
                held[b * 16 + r, c] = tile
    for b in range(8):
        chance = [0.0] * 4
        for c in range(2):
            low = [held[b * 16 + r, c] + side * held[b * 16 + 8 + r, c] for r in range(8)]
            for r, tile in enumerate(walsh(low)):
                state[b * 2 + c, pl.ds(r, 8, stride=8), :] = tile
            for half in range(2):
                rows = [mid * 16 + half * 8 for mid in range(4)]
                for mid, u in enumerate(walsh([state[b * 2 + c, r : r + 8, :] for r in rows])):
                    chance[mid] = chance[mid] + u * u
        for mid in range(4):
            send[b, mid * 8 : mid * 8 + 8, :] = chance[mid] * 0.25


def fourth_kernel(place, held, mine, away, keep, state):
    core = (place[0] & 1) == 0
    far = (place[0] >> 1) == 0
    for b in range(8):
        chance = []
        for c in range(2):
            for r, tile in enumerate(walsh([held[b * 16 + r, c] for r in range(16)])):
                state[b * 2 + c, pl.ds(r // 8 * 64 + r % 8, 8, stride=8), :] = tile
            for top in range(2):
                both = []
                for half in range(2):
                    rows = [top * 64 + mid * 16 + half * 8 for mid in range(4)]
                    both.append(walsh([state[b * 2 + c, r : r + 8, :] for r in rows]))
                for mid, (u, v) in enumerate(zip(*both)):
                    mine[c, b, top, mid * 8 : mid * 8 + 8, :] = jnp.where(core, u, v)
                    away[c, b, top, mid * 8 : mid * 8 + 8, :] = jnp.where(core, v, u)
                    chance.append(u * u + v * v)
        for mid in range(4):
            u = (chance[mid] + chance[8 + mid]) * 0.25
            v = (chance[4 + mid] + chance[12 + mid]) * 0.25
            keep[b, mid * 8 : mid * 8 + 8, :] = jnp.where(far, u, v)


def last_kernel(place, mine, other, out, done):
    core = place[0] & 1
    copies = []
    for c in range(2):
        copies.append(pltpu.make_async_copy(mine.at[c], out.at[c, :, :, core], done.at[0, c]))
        copies.append(pltpu.make_async_copy(other.at[c], out.at[c, :, :, 1 - core], done.at[1, c]))
    for copy in copies:
        copy.start()
    for copy in copies:
        copy.wait()


def here(*dims):
    return pltpu.VMEM(dims, F32)


def near(x):
    return pltpu.with_memory_space_constraint(x, pltpu.VMEM)


VMEM = pl.BlockSpec(memory_space=pltpu.VMEM)
SMEM = pl.BlockSpec(memory_space=pltpu.SMEM)
HBM = pl.BlockSpec(memory_space=pltpu.HBM)
BANK = ("x_hi", "core")
LANE = ("z", "y", "x_lo")
ORDER = ("core", "y", "x_hi", "x_lo", "z")


def shards(amplitudes, energies, diagonal_angles):
    diagonal_angles, bank = lax.optimization_barrier((diagonal_angles, lax.axis_index(BANK)))
    values, angles = pl.pallas_call(
        first_kernel,
        out_shape=(here(128, 3, 8, 128), here(2, 128)),
        in_specs=[HBM] * 3,
        out_specs=(VMEM, VMEM),
        scratch_shapes=[
            here(8, 3, 128, 128),
            here(16, 128, 128),
            pltpu.SemaphoreType.DMA((8, 3)),
            pltpu.SemaphoreType.DMA,
        ],
        name="first",
    )(amplitudes, energies, diagonal_angles)
    values = lax.all_to_all(values.reshape(128, 24, 128), ORDER, 0, 0, tiled=True)
    values = pl.pallas_call(
        second_kernel,
        out_shape=here(128, 2, 8, 128),
        in_specs=[VMEM] * 2,
        out_specs=VMEM,
        scratch_shapes=[here(128, 2, 8, 128), here(2, 64, 16, 128)],
        name="second",
    )(near(values.reshape(128, 3, 8, 128)), near(angles))
    values = lax.all_to_all(values.reshape(128, 16, 128), ORDER, 0, 0, tiled=True)
    place = bank.reshape(1)
    send, held = pl.pallas_call(
        third_kernel,
        out_shape=(here(8, 32, 128), here(128, 2, 8, 128)),
        in_specs=[SMEM, VMEM],
        out_specs=(VMEM, VMEM),
        scratch_shapes=[here(16, 64, 128)],
        name="third",
    )(place, near(values.reshape(128, 2, 8, 128)))
    sent = lax.ppermute(send, "x_hi", [(0, 1), (1, 0)])
    mine, away, keep = pl.pallas_call(
        fourth_kernel,
        out_shape=(here(2, 8, 2, 32, 128), here(2, 8, 2, 32, 128), here(8, 32, 128)),
        in_specs=[SMEM, VMEM],
        out_specs=(VMEM,) * 3,
        scratch_shapes=[here(16, 128, 128)],
        name="fourth",
    )(place, near(held))
    other = lax.ppermute(away, "core", [(0, 1), (1, 0)])
    final = pl.pallas_call(
        last_kernel,
        out_shape=jax.ShapeDtypeStruct((2, 8, 2, 2, 32, 128), F32),
        in_specs=[SMEM, VMEM, VMEM],
        out_specs=HBM,
        scratch_shapes=[pltpu.SemaphoreType.DMA((2, 2))],
        name="last",
    )(place, near(mine), near(other))
    marginal = keep + sent
    return final.reshape(2, 8, 128, 128), marginal


def solution(mesh):
    mesh = Mesh(mesh.devices.reshape(2, 2, 4, 4, 2), BANK + LANE)
    return jax.shard_map(
        shards,
        mesh=mesh,
        in_specs=(P(None, BANK + LANE, None, None), P(BANK + LANE, None, None), P()),
        out_specs=(P(None, BANK + LANE, None, None), P(LANE, BANK, None)),
        check_vma=False,
    )
```

```python
import jax
import jax.numpy as jnp
import numpy as np
from jax import lax
from jax.experimental import pallas as pl
from jax.experimental.pallas import tpu as pltpu
from jax.sharding import Mesh, PartitionSpec as P


F32 = jnp.float32
BF16 = jnp.bfloat16
GROUPS = (3, 5)
SCALE = 2.0**-13


def fit(terms, reach):
    k = np.arange(400)
    x = reach * np.cos(np.pi * (k + 0.5) / 400)
    powers = np.stack([x ** (2 * n + 1) for n in range(terms)], 1)
    scale = np.abs(powers).max(0)
    return [float(c) for c in np.linalg.lstsq(powers / scale, 2 * np.sin(x), rcond=None)[0] / scale]


SIN = fit(5, 1.3)


def turned(re, im, half):
    square = half * half
    sin = jnp.full_like(half, SIN[-1])
    for c in SIN[-2::-1]:
        sin = sin * square + c
    sin = sin * half
    square = sin * sin
    rest = 4.0 - square
    cos, sin = 2.0 - square, sin * (rest * lax.rsqrt(rest))
    return re * cos + im * sin, im * cos - re * sin


def walsh(parts):
    parts, step = list(parts), 1
    while step < len(parts):
        for i in range(len(parts)):
            if not i & step:
                u, v = parts[i], parts[i + step]
                parts[i], parts[i + step] = u + v, u - v
        step *= 2
    return parts


def signs():
    both = lax.broadcasted_iota(jnp.int32, (128, 128), 0) & lax.broadcasted_iota(jnp.int32, (128, 128), 1)
    for shift in (4, 2, 1):
        both = both ^ (both >> shift)
    sign = ((1 - 2 * (both & 1)).astype(F32) * SCALE).astype(BF16)
    return jnp.concatenate([jnp.concatenate([sign, sign], 1), jnp.concatenate([sign, -sign], 1)], 0)


PIECES = 2


def mixed(part, sign):
    rest = jnp.concatenate([part[:64], part[64:]], 1)
    pieces = []
    for _ in range(PIECES):
        pieces.append(rest.astype(BF16))
        rest = rest - pieces[-1].astype(F32)
    both = jnp.dot(jnp.concatenate(pieces, 1), jnp.concatenate([sign] * PIECES, 0), preferred_element_type=F32)
    return walsh(tiles(both[:, :128])) + walsh(tiles(both[:, 128:]))


def tiles(x):
    return [x[r * 8 : r * 8 + 8] for r in range(x.shape[0] // 8)]


def first_kernel(amp, ener, given, out, angle, held, state, arrived, known):
    def copies(b):
        return [
            pltpu.make_async_copy(amp.at[0, b], held.at[b, 0], arrived.at[b, 0]),
            pltpu.make_async_copy(amp.at[1, b], held.at[b, 1], arrived.at[b, 1]),
            pltpu.make_async_copy(ener.at[b], held.at[b, 2], arrived.at[b, 2]),
        ]

    angles = pltpu.make_async_copy(given, angle, known)
    angles.start()
    for b in range(8):
        for copy in copies(b):
            copy.start()
    starts = {sum(GROUPS[:i]): size for i, size in enumerate(GROUPS)}
    sign = signs()
    angles.wait()
    a = angle[0:1, :] * 0.5
    for b in range(8):
        if b in starts:
            for ready in range(b, b + starts[b]):
                for copy in copies(ready):
                    copy.wait()
        re, im = turned(held[b, 0], held[b, 1], a * held[b, 2])
        for c, part in enumerate((re, im)):
            for r, tile in enumerate(mixed(part, sign)):
                state[b * 2 + c, r * 8 : r * 8 + 8, :] = tile
        for top in range(2):
            for low in range(8):
                out[b * 16 + top * 8 + low, 2] = held[b, 2, pl.ds(top * 64 + low, 8, stride=8), :]
            for c in range(2):
                rows = [state[b * 2 + c, pl.ds(top * 64 + low, 8, stride=8), :] for low in range(8)]
                for low, tile in enumerate(walsh(rows)):
                    out[b * 16 + top * 8 + low, c] = tile
    for r in range(16):
        for c in range(2):
            for b, tile in enumerate(walsh([out[b * 16 + r, c] for b in range(8)])):
                out[b * 16 + r, c] = tile


def second_kernel(got, angle, out, held, state):
    sign = signs()
    a = angle[1:2, :] * 0.5
    for r in range(16):
        rows = [r // 8 * 64 + high * 8 + r % 8 for high in range(8)]
        for c in range(2):
            for row, tile in zip(rows, walsh([got[row, c] for row in rows])):
                held[row, c] = tile
    for high in range(8):
        rows = [core * 64 + high * 8 + low for core in range(2) for low in range(8)]
        re = jnp.concatenate(walsh([held[row, 0] for row in rows]), 0)
        im = jnp.concatenate(walsh([held[row, 1] for row in rows]), 0)
        e = jnp.concatenate([got[row, 2] for row in rows], 0)
        re, im = turned(re, im, a * e)
        for c, part in enumerate((re, im)):
            for r, tile in enumerate(mixed(part, sign)):
                state[c, high * 8 + r % 8, pl.ds(r // 8, 8, stride=2), :] = tile
    for low in range(8):
        for c in range(2):
            parts = [state[c, high * 8 + low, r5 * 8 : r5 * 8 + 8, :] for r5 in range(2) for high in range(8)]
            for r, tile in enumerate(walsh(parts)):
                out[r // 8 * 64 + r % 8 * 8 + low, c] = tile


def third_kernel(place, got, send, held, state):
    side = jnp.full((8, 128), (2 * (place[0] >> 1) - 1).astype(F32))
    for r in range(16):
        for c in range(2):
            for b, tile in enumerate(walsh([got[b * 16 + r, c] for b in range(8)])):
                held[b * 16 + r, c] = tile
    for b in range(8):
        chance = [0.0] * 4
        for c in range(2):
            low = [held[b * 16 + r, c] + side * held[b * 16 + 8 + r, c] for r in range(8)]
            for r, tile in enumerate(walsh(low)):
                state[b * 2 + c, pl.ds(r, 8, stride=8), :] = tile
            for half in range(2):
                rows = [mid * 16 + half * 8 for mid in range(4)]
                for mid, u in enumerate(walsh([state[b * 2 + c, r : r + 8, :] for r in rows])):
                    chance[mid] = chance[mid] + u * u
        for mid in range(4):
            send[b, mid * 8 : mid * 8 + 8, :] = chance[mid] * 0.25


def fourth_kernel(place, held, mine, away, keep, state):
    core = (place[0] & 1) == 0
    far = (place[0] >> 1) == 0
    for b in range(8):
        chance = []
        for c in range(2):
            for r, tile in enumerate(walsh([held[b * 16 + r, c] for r in range(16)])):
                state[b * 2 + c, pl.ds(r // 8 * 64 + r % 8, 8, stride=8), :] = tile
            for top in range(2):
                both = []
                for half in range(2):
                    rows = [top * 64 + mid * 16 + half * 8 for mid in range(4)]
                    both.append(walsh([state[b * 2 + c, r : r + 8, :] for r in rows]))
                for mid, (u, v) in enumerate(zip(*both)):
                    mine[c, b, top, mid * 8 : mid * 8 + 8, :] = jnp.where(core, u, v)
                    away[c, b, top, mid * 8 : mid * 8 + 8, :] = jnp.where(core, v, u)
                    chance.append(u * u + v * v)
        for mid in range(4):
            u = (chance[mid] + chance[8 + mid]) * 0.25
            v = (chance[4 + mid] + chance[12 + mid]) * 0.25
            keep[b, mid * 8 : mid * 8 + 8, :] = jnp.where(far, u, v)


def last_kernel(place, mine, other, out, done):
    core = place[0] & 1
    copies = []
    for c in range(2):
        copies.append(pltpu.make_async_copy(mine.at[c], out.at[c, :, :, core], done.at[0, c]))
        copies.append(pltpu.make_async_copy(other.at[c], out.at[c, :, :, 1 - core], done.at[1, c]))
    for copy in copies:
        copy.start()
    for copy in copies:
        copy.wait()


def here(*dims):
    return pltpu.VMEM(dims, F32)


def near(x):
    return pltpu.with_memory_space_constraint(x, pltpu.VMEM)


VMEM = pl.BlockSpec(memory_space=pltpu.VMEM)
SMEM = pl.BlockSpec(memory_space=pltpu.SMEM)
HBM = pl.BlockSpec(memory_space=pltpu.HBM)
BANK = ("x_hi", "core")
LANE = ("z", "y", "x_lo")
ORDER = ("core", "y", "x_hi", "x_lo", "z")


def shards(amplitudes, energies, diagonal_angles):
    diagonal_angles, bank = lax.optimization_barrier((diagonal_angles, lax.axis_index(BANK)))
    values, angles = pl.pallas_call(
        first_kernel,
        out_shape=(here(128, 3, 8, 128), here(2, 128)),
        in_specs=[HBM] * 3,
        out_specs=(VMEM, VMEM),
        scratch_shapes=[
            here(8, 3, 128, 128),
            here(16, 128, 128),
            pltpu.SemaphoreType.DMA((8, 3)),
            pltpu.SemaphoreType.DMA,
        ],
        name="first",
    )(amplitudes, energies, diagonal_angles)
    values = lax.all_to_all(values.reshape(128, 24, 128), ORDER, 0, 0, tiled=True)
    values = pl.pallas_call(
        second_kernel,
        out_shape=here(128, 2, 8, 128),
        in_specs=[VMEM] * 2,
        out_specs=VMEM,
        scratch_shapes=[here(128, 2, 8, 128), here(2, 64, 16, 128)],
        name="second",
    )(near(values.reshape(128, 3, 8, 128)), near(angles))
    values = lax.all_to_all(values.reshape(128, 16, 128), ORDER, 0, 0, tiled=True)
    place = bank.reshape(1)
    send, held = pl.pallas_call(
        third_kernel,
        out_shape=(here(8, 32, 128), here(128, 2, 8, 128)),
        in_specs=[SMEM, VMEM],
        out_specs=(VMEM, VMEM),
        scratch_shapes=[here(16, 64, 128)],
        name="third",
    )(place, near(values.reshape(128, 2, 8, 128)))
    sent = lax.ppermute(send, "x_hi", [(0, 1), (1, 0)])
    mine, away, keep = pl.pallas_call(
        fourth_kernel,
        out_shape=(here(2, 8, 2, 32, 128), here(2, 8, 2, 32, 128), here(8, 32, 128)),
        in_specs=[SMEM, VMEM],
        out_specs=(VMEM,) * 3,
        scratch_shapes=[here(16, 128, 128)],
        name="fourth",
    )(place, near(held))
    other = lax.ppermute(away, "core", [(0, 1), (1, 0)])
    final = pl.pallas_call(
        last_kernel,
        out_shape=jax.ShapeDtypeStruct((2, 8, 2, 2, 32, 128), F32),
        in_specs=[SMEM, VMEM, VMEM],
        out_specs=HBM,
        scratch_shapes=[pltpu.SemaphoreType.DMA((2, 2))],
        name="last",
    )(place, near(mine), near(other))
    marginal = keep + sent
    return final.reshape(2, 8, 128, 128), marginal


def solution(mesh):
    mesh = Mesh(mesh.devices.reshape(2, 2, 4, 4, 2), BANK + LANE)
    return jax.shard_map(
        shards,
        mesh=mesh,
        in_specs=(P(None, BANK + LANE, None, None), P(BANK + LANE, None, None), P()),
        out_specs=(P(None, BANK + LANE, None, None), P(LANE, BANK, None)),
        check_vma=False,
    )
```

```python
import jax
import jax.numpy as jnp
import numpy as np
from jax import lax
from jax.experimental import pallas as pl
from jax.experimental.pallas import tpu as pltpu
from jax.sharding import Mesh, PartitionSpec as P


F32 = jnp.float32
BF16 = jnp.bfloat16
GROUPS = (3, 5)
SCALE = 2.0**-13


def fit(terms, reach):
    k = np.arange(400)
    x = reach * np.cos(np.pi * (k + 0.5) / 400)
    powers = np.stack([x ** (2 * n + 1) for n in range(terms)], 1)
    scale = np.abs(powers).max(0)
    return [float(c) for c in np.linalg.lstsq(powers / scale, 2 * np.sin(x), rcond=None)[0] / scale]


SIN = fit(5, 1.3)


def turned(re, im, half):
    square = half * half
    sin = jnp.full_like(half, SIN[-1])
    for c in SIN[-2::-1]:
        sin = sin * square + c
    sin = sin * half
    square = sin * sin
    rest = 4.0 - square
    cos, sin = 2.0 - square, sin * (rest * lax.rsqrt(rest))
    return re * cos + im * sin, im * cos - re * sin


def walsh(parts):
    parts, step = list(parts), 1
    while step < len(parts):
        for i in range(len(parts)):
            if not i & step:
                u, v = parts[i], parts[i + step]
                parts[i], parts[i + step] = u + v, u - v
        step *= 2
    return parts


def signs():
    both = lax.broadcasted_iota(jnp.int32, (128, 128), 0) & lax.broadcasted_iota(jnp.int32, (128, 128), 1)
    for shift in (4, 2, 1):
        both = both ^ (both >> shift)
    sign = ((1 - 2 * (both & 1)).astype(F32) * SCALE).astype(BF16)
    return jnp.concatenate([jnp.concatenate([sign, sign], 1), jnp.concatenate([sign, -sign], 1)], 0)


PIECES = 2


def mixed(part, sign):
    rest = jnp.concatenate([part[:64], part[64:]], 1)
    pieces = []
    for _ in range(PIECES):
        pieces.append(rest.astype(BF16))
        rest = rest - pieces[-1].astype(F32)
    both = jnp.dot(jnp.concatenate(pieces, 1), jnp.concatenate([sign] * PIECES, 0), preferred_element_type=F32)
    return walsh(tiles(both[:, :128])) + walsh(tiles(both[:, 128:]))


def tiles(x):
    return [x[r * 8 : r * 8 + 8] for r in range(x.shape[0] // 8)]


def first_kernel(amp, ener, given, out, angle, held, state, arrived, known):
    def copies(b):
        return [
            pltpu.make_async_copy(amp.at[0, b], held.at[b, 0], arrived.at[b, 0]),
            pltpu.make_async_copy(amp.at[1, b], held.at[b, 1], arrived.at[b, 1]),
            pltpu.make_async_copy(ener.at[b], held.at[b, 2], arrived.at[b, 2]),
        ]

    angles = pltpu.make_async_copy(given, angle, known)
    angles.start()
    for b in range(8):
        for copy in copies(b):
            copy.start()
    starts = {sum(GROUPS[:i]): size for i, size in enumerate(GROUPS)}
    sign = signs()
    angles.wait()
    a = angle[0:1, :] * 0.5
    for b in range(8):
        if b in starts:
            for ready in range(b, b + starts[b]):
                for copy in copies(ready):
                    copy.wait()
        re, im = turned(held[b, 0], held[b, 1], a * held[b, 2])
        for c, part in enumerate((re, im)):
            for r, tile in enumerate(mixed(part, sign)):
                state[b * 2 + c, r * 8 : r * 8 + 8, :] = tile
        for top in range(2):
            for low in range(8):
                out[b * 16 + top * 8 + low, 2] = held[b, 2, pl.ds(top * 64 + low, 8, stride=8), :]
            for c in range(2):
                rows = [state[b * 2 + c, pl.ds(top * 64 + low, 8, stride=8), :] for low in range(8)]
                for low, tile in enumerate(walsh(rows)):
                    out[b * 16 + top * 8 + low, c] = tile
    for r in range(16):
        for c in range(2):
            for b, tile in enumerate(walsh([out[b * 16 + r, c] for b in range(8)])):
                out[b * 16 + r, c] = tile


def second_kernel(got, angle, out, held, state):
    sign = signs()
    a = angle[1:2, :] * 0.5
    for r in range(16):
        rows = [r // 8 * 64 + high * 8 + r % 8 for high in range(8)]
        for c in range(2):
            for row, tile in zip(rows, walsh([got[row, c] for row in rows])):
                held[row, c] = tile
    for high in range(8):
        rows = [core * 64 + high * 8 + low for core in range(2) for low in range(8)]
        re = jnp.concatenate(walsh([held[row, 0] for row in rows]), 0)
        im = jnp.concatenate(walsh([held[row, 1] for row in rows]), 0)
        e = jnp.concatenate([got[row, 2] for row in rows], 0)
        re, im = turned(re, im, a * e)
        for c, part in enumerate((re, im)):
            for r, tile in enumerate(mixed(part, sign)):
                state[c, high * 8 + r % 8, pl.ds(r // 8, 8, stride=2), :] = tile
    for low in range(8):
        for c in range(2):
            parts = [state[c, high * 8 + low, r5 * 8 : r5 * 8 + 8, :] for r5 in range(2) for high in range(8)]
            for r, tile in enumerate(walsh(parts)):
                out[r // 8 * 64 + r % 8 * 8 + low, c] = tile


def third_kernel(place, got, send, held, state):
    side = jnp.full((8, 128), (2 * (place[0] >> 1) - 1).astype(F32))
    for r in range(8):
        for c in range(2):
            kept = [got[b * 16 + r, c] + side * got[b * 16 + 8 + r, c] for b in range(8)]
            for b, tile in enumerate(walsh(kept)):
                held[b * 8 + r, c] = tile
    for b in range(8):
        chance = [0.0] * 4
        for c in range(2):
            low = [held[b * 8 + r, c] for r in range(8)]
            for r, tile in enumerate(walsh(low)):
                state[b * 2 + c, pl.ds(r, 8, stride=8), :] = tile
            for half in range(2):
                rows = [mid * 16 + half * 8 for mid in range(4)]
                for mid, u in enumerate(walsh([state[b * 2 + c, r : r + 8, :] for r in rows])):
                    chance[mid] = chance[mid] + u * u
        for mid in range(4):
            send[b, mid * 8 : mid * 8 + 8, :] = chance[mid] * 0.25


def fourth_kernel(place, got, mine, away, keep, held, state):
    for r in range(16):
        for c in range(2):
            for b, tile in enumerate(walsh([got[b * 16 + r, c] for b in range(8)])):
                held[b * 16 + r, c] = tile
    core = (place[0] & 1) == 0
    far = (place[0] >> 1) == 0
    for b in range(8):
        chance = []
        for c in range(2):
            for r, tile in enumerate(walsh([held[b * 16 + r, c] for r in range(16)])):
                state[b * 2 + c, pl.ds(r // 8 * 64 + r % 8, 8, stride=8), :] = tile
            for top in range(2):
                both = []
                for half in range(2):
                    rows = [top * 64 + mid * 16 + half * 8 for mid in range(4)]
                    both.append(walsh([state[b * 2 + c, r : r + 8, :] for r in rows]))
                for mid, (u, v) in enumerate(zip(*both)):
                    mine[c, b, top, mid * 8 : mid * 8 + 8, :] = jnp.where(core, u, v)
                    away[c, b, top, mid * 8 : mid * 8 + 8, :] = jnp.where(core, v, u)
                    chance.append(u * u + v * v)
        for mid in range(4):
            u = (chance[mid] + chance[8 + mid]) * 0.25
            v = (chance[4 + mid] + chance[12 + mid]) * 0.25
            keep[b, mid * 8 : mid * 8 + 8, :] = jnp.where(far, u, v)


def last_kernel(place, mine, other, out, done):
    core = place[0] & 1
    copies = []
    for c in range(2):
        copies.append(pltpu.make_async_copy(mine.at[c], out.at[c, :, :, core], done.at[0, c]))
        copies.append(pltpu.make_async_copy(other.at[c], out.at[c, :, :, 1 - core], done.at[1, c]))
    for copy in copies:
        copy.start()
    for copy in copies:
        copy.wait()


def here(*dims):
    return pltpu.VMEM(dims, F32)


def near(x):
    return pltpu.with_memory_space_constraint(x, pltpu.VMEM)


VMEM = pl.BlockSpec(memory_space=pltpu.VMEM)
SMEM = pl.BlockSpec(memory_space=pltpu.SMEM)
HBM = pl.BlockSpec(memory_space=pltpu.HBM)
BANK = ("x_hi", "core")
LANE = ("z", "y", "x_lo")
ORDER = ("core", "x_hi", "x_lo", "y", "z")


def shards(amplitudes, energies, diagonal_angles):
    diagonal_angles, bank = lax.optimization_barrier((diagonal_angles, lax.axis_index(BANK)))
    values, angles = pl.pallas_call(
        first_kernel,
        out_shape=(here(128, 3, 8, 128), here(2, 128)),
        in_specs=[HBM] * 3,
        out_specs=(VMEM, VMEM),
        scratch_shapes=[
            here(8, 3, 128, 128),
            here(16, 128, 128),
            pltpu.SemaphoreType.DMA((8, 3)),
            pltpu.SemaphoreType.DMA,
        ],
        name="first",
    )(amplitudes, energies, diagonal_angles)
    values = lax.all_to_all(values.reshape(128, 24, 128), ORDER, 0, 0, tiled=True)
    values = pl.pallas_call(
        second_kernel,
        out_shape=here(128, 2, 8, 128),
        in_specs=[VMEM] * 2,
        out_specs=VMEM,
        scratch_shapes=[here(128, 2, 8, 128), here(2, 64, 16, 128)],
        name="second",
    )(near(values.reshape(128, 3, 8, 128)), near(angles))
    values = lax.all_to_all(values.reshape(128, 16, 128), ORDER, 0, 0, tiled=True)
    place = bank.reshape(1)
    values = near(values.reshape(128, 2, 8, 128))
    send = pl.pallas_call(
        third_kernel,
        out_shape=here(8, 32, 128),
        in_specs=[SMEM, VMEM],
        out_specs=VMEM,
        scratch_shapes=[here(64, 2, 8, 128), here(16, 64, 128)],
        name="third",
    )(place, values)
    sent = lax.ppermute(send, "x_hi", [(0, 1), (1, 0)])
    mine, away, keep = pl.pallas_call(
        fourth_kernel,
        out_shape=(here(2, 8, 2, 32, 128), here(2, 8, 2, 32, 128), here(8, 32, 128)),
        in_specs=[SMEM, VMEM],
        out_specs=(VMEM,) * 3,
        scratch_shapes=[here(128, 2, 8, 128), here(16, 128, 128)],
        name="fourth",
    )(place, values)
    other = lax.ppermute(away, "core", [(0, 1), (1, 0)])
    final = pl.pallas_call(
        last_kernel,
        out_shape=jax.ShapeDtypeStruct((2, 8, 2, 2, 32, 128), F32),
        in_specs=[SMEM, VMEM, VMEM],
        out_specs=HBM,
        scratch_shapes=[pltpu.SemaphoreType.DMA((2, 2))],
        name="last",
    )(place, near(mine), near(other))
    marginal = keep + sent
    return final.reshape(2, 8, 128, 128), marginal


def solution(mesh):
    mesh = Mesh(mesh.devices.reshape(2, 2, 4, 4, 2), BANK + LANE)
    return jax.shard_map(
        shards,
        mesh=mesh,
        in_specs=(P(None, BANK + LANE, None, None), P(BANK + LANE, None, None), P()),
        out_specs=(P(None, BANK + LANE, None, None), P(LANE, BANK, None)),
        check_vma=False,
    )
```
